1024 devices in a mesh: gx: 64 (over z, core), gy: 16 (over x, y).
Axes of the slice: x: 4, y: 4, z: 32, core: 2. Of those that a mesh axis runs over, the one named last changes fastest.
Arguments:
- suction_potential: float32 [512, 128, 128], P('gx', 'gy'), may hold values from -3 to 0.3
- ground_warmth: float32 [512, 128, 128], P('gx', 'gy'), may hold values from -4 to 4
- ground_category: int32 [512, 128, 128], P('gx', 'gy'), may hold values from 0 to 11
- icebound_flag: int32 [512, 128, 128], P('gx', 'gy'), may hold values 0 or 1
- ground_wetted_permeability: float32 [12], replicated, may hold values from 0.02 to 0.15
- ground_falloff_exponent: float32 [12], replicated, may hold values from 0.3 to 1.5
- camera_skew_per_plane: float32 [4], replicated, may hold values from -1 to 1
- hue_gradient_steepness: float32 [3], replicated, may hold values from 4 to 16
- hue_gradient_middles: float32 [3], replicated, may hold values from 0.1 to 0.4
- camera_distance_ordering: int32 [4, 16], replicated, may hold values from 0 to 15, as said below
Outputs:
- head_out: float32 [512, 128, 128], P('gx', 'gy')
- temp_out: float32 [512, 128, 128], P('gx', 'gy')
- image: float32 [4, 4, 512, 128], P(None, None, 'gx', 'gy')
The draws below stay inside these ranges and needn't reach their ends.
Inputs may be any that keep to these rules, and one draw needn't show every extreme that they name: Each row of camera_distance_ordering names every slab 0 to 15 once.
All inputs are finite; a program needn't handle non-finite values. No bound on the sum of `icebound_flag` on one device may be relied on, other than what follows from the above.
Results may differ from the reference program's by a relative error of at most 0.0003.
Values sent between devices are 32-bit elements; how exact they have to be, the bound alone decides.
A program may use at most 32 MiB of HBM per device.

```python
import math
import jax
import jax.numpy as jnp
from jax import lax

UPRIGHT_COUNT = 128
STEPS = 2
VIEWS = 4
SOILS = 12
EASTWARD_COUNT = 512
NORTHWARD_COUNT = 128
GROUPS = 16


def draw_camera_distance_ordering(key, part):
    view_keys = jax.random.split(jax.random.fold_in(key, 7301), VIEWS)

    def one_row(row_key):
        return jax.random.permutation(row_key, jnp.arange(GROUPS, dtype=jnp.int32))
    return jax.vmap(one_row)(view_keys).astype(jnp.int32)


def touch_ends(entries, rng, smallest, top_value):
    dims = entries.shape
    index_at = [jax.random.randint(jax.random.fold_in(rng, axis), (), 0, dims[axis]) for axis in range(len(dims))]
    entries = entries.at[tuple(index_at)].set(smallest)
    longest = dims.index(max(dims))
    index_at[longest] = (index_at[longest] + 1) % dims[longest]
    return entries.at[tuple(index_at)].set(top_value)


def block_levels(key, extent, cuts, smallest, high):
    factor_of, own = 1.0, jax.random.fold_in(key, 6)
    for dim, blocks in cuts:
        draws = jnp.exp(jax.random.uniform(jax.random.fold_in(own, dim), (blocks,), jnp.float32, smallest / len(cuts), high / len(cuts)))
        factor_of = factor_of * jnp.repeat(draws, extent[dim] // blocks).reshape([-1 if axis == dim else 1 for axis in range(len(extent))])
    return factor_of


def setup_inputs(seed: int = 0) -> dict:
    key_of = jax.random.split(jax.random.key(seed), 11)
    return {
        "suction_potential": jnp.clip(-3.0 + 3.3 * jax.random.uniform(key_of[0], (EASTWARD_COUNT, NORTHWARD_COUNT, UPRIGHT_COUNT), jnp.float32) ** block_levels(key_of[0], (EASTWARD_COUNT, NORTHWARD_COUNT, UPRIGHT_COUNT), ((0, 64), (1, 16)), -0.2, 0.2), -3.0, 0.3),
        "ground_warmth": jnp.clip(jax.random.uniform(key_of[1], (EASTWARD_COUNT, NORTHWARD_COUNT, UPRIGHT_COUNT), jnp.float32, -4.0, 4.0) * block_levels(key_of[1], (EASTWARD_COUNT, NORTHWARD_COUNT, UPRIGHT_COUNT), ((0, 64), (1, 16)), -0.4, 0.0), -4.0, 4.0),
        "ground_category": touch_ends(jax.random.randint(key_of[2], (EASTWARD_COUNT, NORTHWARD_COUNT, UPRIGHT_COUNT), 0, SOILS), jax.random.fold_in(key_of[2], 1), 0, SOILS - 1).astype(jnp.int32),
        "icebound_flag": touch_ends((jax.random.randint(key_of[3], (EASTWARD_COUNT, NORTHWARD_COUNT, UPRIGHT_COUNT), 0, 2) < 1).astype(jnp.int32), jax.random.fold_in(key_of[3], 1), 0, 1),
        "ground_wetted_permeability": jnp.clip(jnp.exp(jax.random.uniform(key_of[4], (SOILS,), jnp.float32, math.log(0.02), math.log(0.15))), 0.02, 0.15),
        "ground_falloff_exponent": jnp.clip(jnp.exp(jax.random.uniform(key_of[5], (SOILS,), jnp.float32, math.log(0.3), math.log(1.5))), 0.3, 1.5),
        "camera_skew_per_plane": jnp.clip(jax.random.uniform(key_of[6], (VIEWS,), jnp.float32, -1.0, 1.0), -1.0, 1.0),
        "hue_gradient_steepness": jnp.clip(jnp.exp(jax.random.uniform(key_of[7], (3,), jnp.float32, math.log(4.0), math.log(16.0))), 4.0, 16.0),
        "hue_gradient_middles": jnp.clip(jax.random.uniform(key_of[8], (3,), jnp.float32, 0.1, 0.4), 0.1, 0.4),
        "camera_distance_ordering": draw_camera_distance_ordering(jax.random.fold_in(key_of[10], 71), 0),
    }


IMPEDANCE = 4.0
DIFFUSE = 0.12


def voxel_index_map(ground_category, table):
    total = jnp.zeros(ground_category.shape, jnp.float32)
    for number in range(table.shape[0]):
        total = total + jnp.where(ground_category == number, table[number], jnp.float32(0.0))
    return total


def advance(evolving_arrays, first_row, first_col, rows_all, cols_all):
    suction_potential, temp, conduct_sat, alpha, ice = evolving_arrays
    conduct = conduct_sat * jnp.exp(alpha * jnp.minimum(suction_potential, 0.0)) * jnp.exp(-IMPEDANCE * ice * jax.nn.sigmoid(-2.0 * temp))
    global_rows = first_row + jnp.arange(suction_potential.shape[0], dtype=jnp.int32)
    global_cols = first_col + jnp.arange(suction_potential.shape[1], dtype=jnp.int32)
    open_rows = ((global_rows[:-1] >= 0) & (global_rows[1:] <= rows_all - 1))[:, None, None]
    open_cols = ((global_cols[:-1] >= 0) & (global_cols[1:] <= cols_all - 1))[None, :, None]
    flux_rows = jnp.where(open_rows, 0.5 * (conduct[1:] + conduct[:-1]) * (suction_potential[1:] - suction_potential[:-1]), 0.0)
    flux_cols = jnp.where(open_cols, 0.5 * (conduct[:, 1:] + conduct[:, :-1]) * (suction_potential[:, 1:] - suction_potential[:, :-1]), 0.0)
    flux_up = 0.5 * (conduct[..., 1:] + conduct[..., :-1]) * (suction_potential[..., 1:] - suction_potential[..., :-1] + 1.0)
    zeros_up = jnp.zeros(suction_potential.shape[:2] + (1,), suction_potential.dtype)
    change_up = jnp.concatenate([flux_up, zeros_up], 2) - jnp.concatenate([zeros_up, flux_up], 2)
    change = (flux_rows[1:, 1:-1] - flux_rows[:-1, 1:-1]) + (flux_cols[1:-1, 1:] - flux_cols[1:-1, :-1]) + change_up[1:-1, 1:-1]
    inside = ((global_rows[1:-1] >= 0) & (global_rows[1:-1] <= rows_all - 1))[:, None, None] & ((global_cols[1:-1] >= 0) & (global_cols[1:-1] <= cols_all - 1))[None, :, None]
    head_new = jnp.where(inside, suction_potential[1:-1, 1:-1] + change, 0.0)
    vertical = jnp.concatenate([temp[..., 1:], zeros_up], 2) + jnp.concatenate([zeros_up, temp[..., :-1]], 2)
    laplace = temp[2:, 1:-1] + temp[:-2, 1:-1] + temp[1:-1, 2:] + temp[1:-1, :-2] + vertical[1:-1, 1:-1] - 6.0 * temp[1:-1, 1:-1]
    temp_new = jnp.where(inside, temp[1:-1, 1:-1] + DIFFUSE * laplace, 0.0)
    return (head_new, temp_new, conduct_sat[1:-1, 1:-1], alpha[1:-1, 1:-1], ice[1:-1, 1:-1])


def moisture(suction_potential):
    return 0.05 + 0.4 * jnp.exp(0.8 * jnp.minimum(suction_potential, 0.0))


def render(theta, first_plane, planes_all, groups, tilt, gain, middle):
    depth_z = theta.shape[2]
    planes = first_plane + jnp.arange(theta.shape[1], dtype=jnp.int32)
    shift = tilt * (planes.astype(jnp.float32) - 0.5 * planes_all)
    wrapped = shift - depth_z * jnp.floor(shift / depth_z)
    base = jnp.floor(wrapped)
    frac = wrapped - base
    lower = (jnp.arange(depth_z, dtype=jnp.int32)[None, :] + base.astype(jnp.int32)[:, None]) % depth_z
    upper = (lower + 1) % depth_z
    lower_vals = jnp.take_along_axis(theta, jnp.broadcast_to(lower[None], theta.shape), axis=2)
    upper_vals = jnp.take_along_axis(theta, jnp.broadcast_to(upper[None], theta.shape), axis=2)
    sample = (1.0 - frac)[None, :, None] * lower_vals + frac[None, :, None] * upper_vals
    shape_four = (theta.shape[0], groups, theta.shape[1] // groups, depth_z)
    sample = sample.reshape(shape_four)
    optical = sample * (8.0 / planes_all)
    before = jnp.cumsum(optical, axis=2) - optical
    weight = (1.0 - jnp.exp(-optical)) * jnp.exp(-before)
    layers = [jnp.sum(jax.nn.sigmoid(gain[color] * (sample - middle[color])) * weight, axis=2) for color in range(3)]
    layers.append(jnp.sum(optical, axis=2))
    return jnp.stack(layers, 0).transpose(2, 0, 1, 3)


def composite(pieces, ranks):
    in_front = (ranks[None, :] < ranks[:, None]).astype(jnp.float32)
    depth = pieces[:, 3]
    front = jnp.einsum('ij,jxz->ixz', in_front, depth, precision=lax.Precision.HIGHEST)
    color = jnp.sum(jnp.exp(-front)[:, None] * pieces[:, :3], axis=0)
    opacity = 1.0 - jnp.exp(-jnp.sum(depth, axis=0))
    return jnp.concatenate([color, opacity[None]], 0)


def reference(suction_potential, ground_warmth, ground_category, icebound_flag, ground_wetted_permeability, ground_falloff_exponent, camera_skew_per_plane, hue_gradient_steepness, hue_gradient_middles, camera_distance_ordering):
    evolving_arrays = (suction_potential, ground_warmth, voxel_index_map(ground_category, ground_wetted_permeability), voxel_index_map(ground_category, ground_falloff_exponent), icebound_flag.astype(jnp.float32))
    for number in range(STEPS):
        padded = tuple(jnp.pad(field, ((1, 1), (1, 1), (0, 0))) for field in evolving_arrays)
        evolving_arrays = advance(padded, -1, -1, EASTWARD_COUNT, NORTHWARD_COUNT)
    theta = moisture(evolving_arrays[0])

    def one_view(item):
        tilt, ranks = item
        pieces = render(theta, 0, NORTHWARD_COUNT, GROUPS, tilt, hue_gradient_steepness, hue_gradient_middles)
        return composite(pieces, ranks)

    image = lax.map(one_view, (camera_skew_per_plane, camera_distance_ordering))
    return evolving_arrays[0], evolving_arrays[1], image
```

```python
import functools

import jax
import jax.numpy as jnp
from jax import lax
from jax.experimental import pallas as pl
from jax.experimental.pallas import tpu as pltpu
from jax.sharding import PartitionSpec as P

MESH = pl.DeviceIdType.MESH
SOILS = 12
VIEWS = 4
SIDE = 8
DEPTH = 128
GROUPS = 16
DIFFUSE = 0.12
F32 = jnp.float32


def lookup(category, table):
    total = jnp.full(category.shape, table[0], F32)
    for number in range(1, SOILS):
        total = jnp.where(category == number, table[number], total)
    return total


def conductivity(head, temp, ks, alpha, ice):
    return ks * jnp.exp(alpha * jnp.minimum(head, 0.0) + 2.0 * ice * (jnp.tanh(temp) - 1.0))


def vertical(head, temp, conduct, lane):
    above = pltpu.roll(head, DEPTH - 1, 1)
    conduct_above = pltpu.roll(conduct, DEPTH - 1, 1)
    flux = jnp.where(lane < DEPTH - 1, (conduct + conduct_above) * (above - head + 1.0), 0.0)
    change = flux - pltpu.roll(flux, 1, 1)
    warm = jnp.where(lane < DEPTH - 1, pltpu.roll(temp, DEPTH - 1, 1), 0.0) + jnp.where(
        lane > 0, pltpu.roll(temp, 1, 1), 0.0
    )
    return change, warm


def kernel(
    gx_count,
    gy_count,
    head_in,
    temp_in,
    cat_in,
    ice_in,
    ks_in,
    alpha_in,
    skew_in,
    steep_in,
    mid_in,
    order_in,
    head_out,
    temp_out,
    image_out,
    head_a,
    temp_a,
    cat_a,
    ice_a,
    ks_s,
    alpha_s,
    skew_s,
    steep_s,
    mid_s,
    order_s,
    y_send,
    y_recv,
    x_send,
    x_recv,
    c_send,
    c_recv,
    ghost,
    head_v,
    temp_v,
    piece_send,
    piece_recv,
    image_v,
    in_sem,
    par_sem,
    halo_send_sem,
    halo_recv_sem,
    piece_send_sem,
    piece_recv_sem,
    out_sem,
):
    gx, gy = lax.axis_index("gx"), lax.axis_index("gy")
    gx_lo, gx_hi = lax.rem(gx + gx_count - 1, gx_count), lax.rem(gx + 1, gx_count)
    gy_lo, gy_hi = lax.rem(gy + gy_count - 1, gy_count), lax.rem(gy + 1, gy_count)

    loads = [
        pltpu.make_async_copy(src, dst, in_sem.at[number])
        for number, (src, dst) in enumerate(
            ((head_in, head_a), (temp_in, temp_a), (cat_in, cat_a), (ice_in, ice_a))
        )
    ]
    params = [
        pltpu.make_async_copy(src, dst, par_sem.at[number])
        for number, (src, dst) in enumerate(
            (
                (ks_in, ks_s),
                (alpha_in, alpha_s),
                (skew_in, skew_s),
                (steep_in, steep_s),
                (mid_in, mid_s),
                (order_in, order_s),
            )
        )
    ]
    for copy in params[:2] + loads + params[2:]:
        copy.start()

    px, py = lax.div(gy, 4), lax.rem(gy, 4)
    shifts = sorted(
        ((dx, dy) for dx in range(4) for dy in range(4) if (dx, dy) != (0, 0)),
        key=lambda d: -(min(d[0], 4 - d[0]) + min(d[1], 4 - d[1])),
    )
    peers = [lax.rem(px + dx, 4) * 4 + lax.rem(py + dy, 4) for dx, dy in shifts]
    corners = ((gx_lo, gy_lo), (gx_lo, gy_hi), (gx_hi, gy_lo), (gx_hi, gy_hi))

    barrier = pltpu.get_barrier_semaphore()
    greeted = [(gx, peer) for peer in peers] + [*corners, (gx_lo, gy), (gx_hi, gy)]
    for device in greeted:
        pl.semaphore_signal(barrier, inc=1, device_id=device, device_id_type=MESH)

    row = lax.broadcasted_iota(jnp.int32, (SIDE, DEPTH), 0)
    lane = lax.broadcasted_iota(jnp.int32, (SIDE, DEPTH), 1)
    first, last = row == 0, row == SIDE - 1

    for copy in params[:2]:
        copy.wait()
    for copy in loads:
        copy.wait()

    def across(ref, y):
        return ref[pl.ds(y, SIDE, stride=SIDE), :]

    def tile(ref, x):
        return ref[pl.ds(x * SIDE, SIDE), :]

    head = [across(head_a, y) for y in range(SIDE)]
    temp = [across(temp_a, y) for y in range(SIDE)]
    category = [across(cat_a, y) for y in range(SIDE)]
    ice = [across(ice_a, y).astype(F32) for y in range(SIDE)]
    ks = [lookup(category[y], ks_s) for y in range(SIDE)]
    alpha = [lookup(category[y], alpha_s) for y in range(SIDE)]
    conduct = [
        conductivity(head[y], temp[y], ks[y], alpha[y], ice[y]) for y in range(SIDE)
    ]
    edge = {}
    for x in (0, 1, SIDE - 2, SIDE - 1):
        h, t, c = tile(head_a, x), tile(temp_a, x), tile(cat_a, x)
        i = tile(ice_a, x).astype(F32)
        k = conductivity(h, t, lookup(c, ks_s), lookup(c, alpha_s), i)
        edge[x] = (h, t, c.astype(F32), i, k)

    for side, (near, far) in enumerate(((0, 1), (SIDE - 1, SIDE - 2))):
        parts = (
            head[near],
            temp[near],
            category[near].astype(F32),
            ice[near],
            head[far],
            temp[far],
            conduct[far],
        )
        for number, part in enumerate(parts):
            y_send[side, pl.ds(number * SIDE, SIDE), :] = part
        parts = (*edge[near][:4], edge[far][0], edge[far][1], edge[far][4])
        for number, part in enumerate(parts):
            x_send[side, pl.ds(number * SIDE, SIDE), :] = part
    for number, (x, y) in enumerate(((0, 0), (0, 7), (7, 0), (7, 7))):
        for field, part in enumerate((head[y], temp[y], conduct[y], conduct[y])):
            c_send[number, pl.ds(field, 1), :] = part[x : x + 1, :]

    pl.semaphore_wait(barrier, len(greeted))

    def remote(src, dst, number, device):
        return pltpu.make_async_remote_copy(
            src_ref=src,
            dst_ref=dst,
            send_sem=halo_send_sem.at[number],
            recv_sem=halo_recv_sem.at[number],
            device_id=device,
            device_id_type=MESH,
        )

    for number, device in enumerate(corners):
        remote(c_send.at[number], c_recv.at[3 - number], 0, device).start()
    remote(y_send.at[0], y_recv.at[1], 1, (gx, gy_lo)).start()
    remote(y_send.at[1], y_recv.at[0], 1, (gx, gy_hi)).start()
    remote(x_send.at[0], x_recv.at[1], 2, (gx_lo, gy)).start()
    remote(x_send.at[1], x_recv.at[0], 2, (gx_hi, gy)).start()

    for copy in params[2:]:
        copy.wait()

    has_x = (gx > 0, gx < gx_count - 1)
    has_y = (gy > 0, gy < gy_count - 1)
    x_open = (jnp.logical_or(row > 0, has_x[0]), jnp.logical_or(row < SIDE - 1, has_x[1]))
    y_open = (jnp.logical_or(row > 0, has_y[0]), jnp.logical_or(row < SIDE - 1, has_y[1]))

    own_vertical = [vertical(head[y], temp[y], conduct[y], lane) for y in range(SIDE)]

    whole = (
        remote(c_send, c_recv, 0, (gx, gy_lo)),
        remote(y_send, y_recv, 1, (gx, gy_lo)),
        remote(x_send, x_recv, 2, (gx, gy_lo)),
    )
    for copy in whole:
        copy.wait_recv()

    def along_rows(value, before, after):
        return (
            jnp.where(first, before, pltpu.roll(value, 1, 0)),
            jnp.where(last, after, pltpu.roll(value, SIDE - 1, 0)),
        )

    def change_rows(head_, conduct_, temp_, ends, opened):
        (h_lo, t_lo, k_lo), (h_hi, t_hi, k_hi) = ends
        heads = along_rows(head_, h_lo, h_hi)
        temps = along_rows(temp_, t_lo, t_hi)
        conducts = along_rows(conduct_, k_lo, k_hi)
        total = sum(
            jnp.where(opened[s], (conduct_ + conducts[s]) * (heads[s] - head_), 0.0)
            for s in range(2)
        )
        return total, temps[0] + temps[1]

    def y_part(side, number):
        return y_recv[side, pl.ds(number * SIDE, SIDE), :]

    def x_part(side, number):
        return x_recv[side, pl.ds(number * SIDE, SIDE), :]

    def warm_if(present, value):
        return jnp.where(present, value, 0.0)

    def corner(xs, ys):
        number = 2 * xs + ys
        return (
            c_recv[number, pl.ds(0, 1), :],
            warm_if(jnp.logical_and(has_x[xs], has_y[ys]), c_recv[number, pl.ds(1, 1), :]),
            c_recv[number, pl.ds(2, 1), :],
        )

    y_ghost, x_ghost = [], []
    for part_of, present, dest in ((y_part, has_y, y_ghost), (x_part, has_x, x_ghost)):
        for side in range(2):
            h, t, c, i = (part_of(side, number) for number in range(4))
            k_s, a = lookup(c, ks_s), lookup(c, alpha_s)
            k = conductivity(h, t, k_s, a, i)
            far = tuple(part_of(side, number) for number in range(4, 7))
            dest.append((h, warm_if(present[side], t), k, k_s, a, i, far))

    for side in range(2):
        for field in range(3):
            ghost[side, field] = x_ghost[side][field]

    def step(h, t, change, warm):
        return h + 0.5 * change, t + DIFFUSE * (warm - 6.0 * t)

    def face(k_a, h_a, k_b, h_b):
        return (k_a + k_b) * (h_b - h_a)

    def ghost_step(cell, inner, ends, opened, present):
        h, t, k, k_s, a, i, far = cell
        change, warm = vertical(h, t, k, lane)
        rows, rows_warm = change_rows(h, k, t, ends, opened)
        change = change + rows + face(k, h, far[2], far[0]) + face(k, h, inner[2], inner[0])
        warm = warm + rows_warm + far[1] + inner[1]
        h, t = step(h, t, change, warm)
        return h, warm_if(present, t), conductivity(h, t, k_s, a, i)

    y_next = [
        ghost_step(
            y_ghost[side],
            (head[y], temp[y], conduct[y]),
            (corner(0, side), corner(1, side)),
            x_open,
            has_y[side],
        )
        for side, y in ((0, 0), (1, SIDE - 1))
    ]
    x_next = [
        ghost_step(
            x_ghost[side],
            (edge[x][0], edge[x][1], edge[x][4]),
            (corner(side, 0), corner(side, 1)),
            y_open,
            has_x[side],
        )
        for side, x in ((0, 0), (1, SIDE - 1))
    ]
    for side in range(2):
        for field in range(3):
            ghost[2 + side, field] = x_next[side][field]

    def main_step(head_, temp_, conduct_, lows, highs, slot, verticals):
        hs = [lows[0], *head_, highs[0]]
        ts = [lows[1], *temp_, highs[1]]
        ks_ = [lows[2], *conduct_, highs[2]]
        faces = [face(ks_[y], hs[y], ks_[y + 1], hs[y + 1]) for y in range(SIDE + 1)]
        faces[0] = jnp.where(has_y[0], faces[0], 0.0)
        faces[SIDE] = jnp.where(has_y[1], faces[SIDE], 0.0)
        result = []
        for y in range(SIDE):
            ends = tuple(
                tuple(ghost[slot + side, field, pl.ds(y, 1), :] for field in range(3))
                for side in range(2)
            )
            rows, rows_warm = change_rows(head_[y], conduct_[y], temp_[y], ends, x_open)
            change, warm = verticals[y]
            change = change + rows + faces[y + 1] - faces[y]
            warm = warm + rows_warm + ts[y] + ts[y + 2]
            result.append(step(head_[y], temp_[y], change, warm))
        return [r[0] for r in result], [r[1] for r in result]

    head, temp = main_step(head, temp, conduct, y_ghost[0], y_ghost[1], 0, own_vertical)
    conduct = [
        conductivity(head[y], temp[y], ks[y], alpha[y], ice[y]) for y in range(SIDE)
    ]
    verticals = [vertical(head[y], temp[y], conduct[y], lane) for y in range(SIDE)]
    head, temp = main_step(head, temp, conduct, y_next[0], y_next[1], 2, verticals)

    for y in range(SIDE):
        head_v[pl.ds(y, SIDE, stride=SIDE), :] = head[y]
        temp_v[pl.ds(y, SIDE, stride=SIDE), :] = temp[y]
    stores = [
        pltpu.make_async_copy(head_v, head_out, out_sem.at[0]),
        pltpu.make_async_copy(temp_v, temp_out, out_sem.at[1]),
    ]
    for copy in stores:
        copy.start()

    theta = [0.05 + 0.4 * jnp.exp(0.8 * jnp.minimum(h, 0.0)) for h in head]
    planes_all = gy_count * SIDE
    layers = []
    for view in range(VIEWS):
        clear = None
        sums = [None] * 3
        depth = None
        for y in range(SIDE):
            shift = skew_s[view] * ((gy * SIDE + y).astype(F32) - 0.5 * planes_all)
            wrapped = shift - DEPTH * jnp.floor(shift * (1.0 / DEPTH))
            base = jnp.floor(wrapped)
            part = wrapped - base
            turn = lax.rem(2 * DEPTH - base.astype(jnp.int32), DEPTH)
            lower = pltpu.roll(theta[y], turn, 1)
            upper = pltpu.roll(lower, DEPTH - 1, 1)
            sample = (1.0 - part) * lower + part * upper
            optical = sample * (8.0 / planes_all)
            passed = jnp.exp(-optical)
            after = passed if clear is None else clear * passed
            weight = (1.0 if clear is None else clear) - after
            clear = after
            depth = optical if depth is None else depth + optical
            for color in range(3):
                term = weight * jnp.tanh((0.5 * steep_s[color]) * (sample - mid_s[color]))
                sums[color] = term if sums[color] is None else sums[color] + term
        layers += [0.5 * ((1.0 - clear) + total) for total in sums]
        layers.append(depth)
    piece_send[...] = jnp.transpose(jnp.concatenate(layers, 0))

    def exchange(src, dst, device):
        return pltpu.make_async_remote_copy(
            src_ref=src,
            dst_ref=dst,
            send_sem=piece_send_sem,
            recv_sem=piece_recv_sem,
            device_id=device,
            device_id_type=MESH,
        )

    for peer in peers:
        exchange(
            piece_send.at[pl.ds(pl.multiple_of(peer * SIDE, SIDE), SIDE)],
            piece_recv.at[gy],
            (gx, peer),
        ).start()
    piece_recv[gy] = piece_send[pl.ds(pl.multiple_of(gy * SIDE, SIDE), SIDE), :]

    view_of = lax.div(lane, 4 * SIDE)
    kind_of = lax.rem(lax.div(lane, SIDE), 4)
    ranks = []
    for group in range(GROUPS):
        rank = jnp.full((SIDE, DEPTH), order_s[0, group], jnp.int32)
        for view in range(1, VIEWS):
            rank = jnp.where(view_of == view, order_s[view, group], rank)
        ranks.append(rank)
    is_depth = kind_of == 3

    exchange_in = pltpu.make_async_remote_copy(
        src_ref=piece_recv.at[pl.ds(0, GROUPS - 1)],
        dst_ref=piece_recv.at[pl.ds(0, GROUPS - 1)],
        send_sem=piece_send_sem,
        recv_sem=piece_recv_sem,
        device_id=(gx, gy_lo),
        device_id_type=MESH,
    )
    exchange_in.wait_recv()

    depths = []
    for group in range(GROUPS):
        value = jnp.where(is_depth, piece_recv[group], 0.0)
        value = value + pltpu.roll(value, DEPTH - SIDE, 1)
        depths.append(value + pltpu.roll(value, DEPTH - 2 * SIDE, 1))
    fronts = [jnp.zeros((SIDE, DEPTH), F32)] * GROUPS
    for one in range(GROUPS):
        for two in range(one + 1, GROUPS):
            before = ranks[two] < ranks[one]
            fronts[one] = fronts[one] + jnp.where(before, depths[two], 0.0)
            fronts[two] = fronts[two] + jnp.where(before, 0.0, depths[one])
    color = sum(jnp.exp(-fronts[group]) * piece_recv[group] for group in range(GROUPS))
    opaque = 1.0 - jnp.exp(-sum(depths))
    image_v[...] = jnp.transpose(jnp.where(is_depth, opaque, color))
    stores.append(pltpu.make_async_copy(image_v, image_out, out_sem.at[2]))
    stores[2].start()
    for copy in whole:
        copy.wait_send()
    exchange_in.wait_send()
    for copy in stores:
        copy.wait()


def shards(head, temp, category, ice, *params):
    gx_count, gy_count = lax.axis_size("gx"), lax.axis_size("gy")
    rows = SIDE * SIDE
    flat = [a.reshape(rows, DEPTH) for a in (head, temp, category, ice)]
    vmem = pltpu.VMEM
    dma = pltpu.SemaphoreType.DMA
    head, temp, image = pl.pallas_call(
        functools.partial(kernel, gx_count, gy_count),
        out_shape=(
            jax.ShapeDtypeStruct((rows, DEPTH), F32),
            jax.ShapeDtypeStruct((rows, DEPTH), F32),
            jax.ShapeDtypeStruct((DEPTH, SIDE), F32),
        ),
        in_specs=[pl.BlockSpec(memory_space=pl.ANY)] * 10,
        out_specs=[pl.BlockSpec(memory_space=pl.ANY)] * 3,
        scratch_shapes=[
            vmem((rows, DEPTH), F32),
            vmem((rows, DEPTH), F32),
            vmem((rows, DEPTH), jnp.int32),
            vmem((rows, DEPTH), jnp.int32),
            pltpu.SMEM((SOILS,), F32),
            pltpu.SMEM((SOILS,), F32),
            pltpu.SMEM((VIEWS,), F32),
            pltpu.SMEM((3,), F32),
            pltpu.SMEM((3,), F32),
            pltpu.SMEM((VIEWS, GROUPS), jnp.int32),
            vmem((2, 7 * SIDE, DEPTH), F32),
            vmem((2, 7 * SIDE, DEPTH), F32),
            vmem((2, 7 * SIDE, DEPTH), F32),
            vmem((2, 7 * SIDE, DEPTH), F32),
            vmem((4, 4, DEPTH), F32),
            vmem((4, 4, DEPTH), F32),
            vmem((4, 3, SIDE, DEPTH), F32),
            vmem((rows, DEPTH), F32),
            vmem((rows, DEPTH), F32),
            vmem((DEPTH, DEPTH), F32),
            vmem((GROUPS, SIDE, DEPTH), F32),
            vmem((DEPTH, SIDE), F32),
            dma((4,)),
            dma((6,)),
            dma((3,)),
            dma((3,)),
            dma(()),
            dma(()),
            dma((3,)),
        ],
        compiler_params=pltpu.CompilerParams(collective_id=0, has_side_effects=True),
        name="step_and_view",
    )(*flat, *params)
    shape = (SIDE, SIDE, DEPTH)
    return head.reshape(shape), temp.reshape(shape), image.reshape(VIEWS, 4, SIDE, SIDE)


def solution(mesh):
    block = P("gx", "gy", None)
    return jax.shard_map(
        shards,
        mesh=mesh,
        in_specs=(block,) * 4 + (P(),) * 6,
        out_specs=(block, block, P(None, None, "gx", "gy")),
        check_vma=False,
    )
```

```python
import functools

import jax
import jax.numpy as jnp
from jax import lax
from jax.experimental import pallas as pl
from jax.experimental.pallas import tpu as pltpu
from jax.sharding import PartitionSpec as P

MESH = pl.DeviceIdType.MESH
SOILS = 12
VIEWS = 4
SIDE = 8
DEPTH = 128
GROUPS = 16
DIFFUSE = 0.12
F32 = jnp.float32


def lookup(category, table):
    total = jnp.full(category.shape, table[0], F32)
    for number in range(1, SOILS):
        total = jnp.where(category == number, table[number], total)
    return total


def conductivity(head, temp, ks, alpha, ice):
    return ks * jnp.exp(alpha * jnp.minimum(head, 0.0) + 2.0 * ice * (jnp.tanh(temp) - 1.0))


def vertical(head, temp, conduct, lane):
    above = pltpu.roll(head, DEPTH - 1, 1)
    conduct_above = pltpu.roll(conduct, DEPTH - 1, 1)
    flux = jnp.where(lane < DEPTH - 1, (conduct + conduct_above) * (above - head + 1.0), 0.0)
    change = flux - pltpu.roll(flux, 1, 1)
    warm = jnp.where(lane < DEPTH - 1, pltpu.roll(temp, DEPTH - 1, 1), 0.0) + jnp.where(
        lane > 0, pltpu.roll(temp, 1, 1), 0.0
    )
    return change, warm


def kernel(
    gx_count,
    gy_count,
    head_in,
    temp_in,
    cat_in,
    ice_in,
    ks_in,
    alpha_in,
    skew_in,
    steep_in,
    mid_in,
    order_in,
    head_v,
    temp_v,
    image_v,
    head_a,
    temp_a,
    cat_a,
    ice_a,
    ks_s,
    alpha_s,
    skew_s,
    steep_s,
    mid_s,
    order_s,
    y_send,
    y_recv,
    x_send,
    x_recv,
    c_send,
    c_recv,
    ghost,
    piece_send,
    piece_recv,
    in_sem,
    par_sem,
    halo_send_sem,
    halo_recv_sem,
    piece_send_sem,
    piece_recv_sem,
):
    gx, gy = lax.axis_index("gx"), lax.axis_index("gy")
    gx_lo, gx_hi = lax.rem(gx + gx_count - 1, gx_count), lax.rem(gx + 1, gx_count)
    gy_lo, gy_hi = lax.rem(gy + gy_count - 1, gy_count), lax.rem(gy + 1, gy_count)

    loads = [
        pltpu.make_async_copy(src, dst, in_sem.at[number])
        for number, (src, dst) in enumerate(
            ((head_in, head_a), (temp_in, temp_a), (cat_in, cat_a), (ice_in, ice_a))
        )
    ]
    params = [
        pltpu.make_async_copy(src, dst, par_sem.at[number])
        for number, (src, dst) in enumerate(
            (
                (ks_in, ks_s),
                (alpha_in, alpha_s),
                (skew_in, skew_s),
                (steep_in, steep_s),
                (mid_in, mid_s),
                (order_in, order_s),
            )
        )
    ]
    for copy in params[:2] + loads + params[2:]:
        copy.start()

    px, py = lax.div(gy, 4), lax.rem(gy, 4)
    shifts = sorted(
        ((dx, dy) for dx in range(4) for dy in range(4) if (dx, dy) != (0, 0)),
        key=lambda d: -(min(d[0], 4 - d[0]) + min(d[1], 4 - d[1])),
    )
    peers = [lax.rem(px + dx, 4) * 4 + lax.rem(py + dy, 4) for dx, dy in shifts]

    barrier = pltpu.get_barrier_semaphore()

    def greet(device):
        pl.semaphore_signal(barrier, inc=1, device_id=device, device_id_type=MESH)

    has_x = (gx > 0, gx < gx_count - 1)
    has_y = (gy > 0, gy < gy_count - 1)
    for side, x in enumerate((gx_lo, gx_hi)):

        @pl.when(has_x[side])
        def _():
            for y in (gy_lo, gy_hi, gy):
                greet((x, y))

    for peer in peers:
        greet((gx, peer))

    row = lax.broadcasted_iota(jnp.int32, (SIDE, DEPTH), 0)
    lane = lax.broadcasted_iota(jnp.int32, (SIDE, DEPTH), 1)
    first, last = row == 0, row == SIDE - 1

    for copy in params[:2]:
        copy.wait()
    for copy in loads:
        copy.wait()

    def across(ref, y):
        return ref[pl.ds(y, SIDE, stride=SIDE), :]

    def tile(ref, x):
        return ref[pl.ds(x * SIDE, SIDE), :]

    head = [across(head_a, y) for y in range(SIDE)]
    temp = [across(temp_a, y) for y in range(SIDE)]
    category = [across(cat_a, y) for y in range(SIDE)]
    ice = [across(ice_a, y).astype(F32) for y in range(SIDE)]
    ks = [lookup(category[y], ks_s) for y in range(SIDE)]
    alpha = [lookup(category[y], alpha_s) for y in range(SIDE)]
    conduct = [
        conductivity(head[y], temp[y], ks[y], alpha[y], ice[y]) for y in range(SIDE)
    ]
    edge = {}
    for x in (0, 1, SIDE - 2, SIDE - 1):
        h, t, c = tile(head_a, x), tile(temp_a, x), tile(cat_a, x)
        i = tile(ice_a, x).astype(F32)
        k = conductivity(h, t, lookup(c, ks_s), lookup(c, alpha_s), i)
        edge[x] = (h, t, c.astype(F32), i, k)

    for side, (near, far) in enumerate(((0, 1), (SIDE - 1, SIDE - 2))):
        parts = (
            head[near],
            temp[near],
            category[near].astype(F32),
            ice[near],
            head[far],
            temp[far],
            conduct[far],
        )
        for number, part in enumerate(parts):
            y_send[side, pl.ds(number * SIDE, SIDE), :] = part
        parts = (*edge[near][:4], edge[far][0], edge[far][1], edge[far][4])
        for number, part in enumerate(parts):
            x_send[side, pl.ds(number * SIDE, SIDE), :] = part
    for number, (x, y) in enumerate(((0, 0), (0, 7), (7, 0), (7, 7))):
        for field, part in enumerate((head[y], temp[y], conduct[y], conduct[y])):
            c_send[number // 2, number % 2, pl.ds(field, 1), :] = part[x : x + 1, :]

    one_sided = jnp.logical_or(gx == 0, gx == gx_count - 1)
    pl.semaphore_wait(barrier, len(peers) + jnp.where(one_sided, 3, 6))

    def remote(src, dst, mine, theirs, device):
        return pltpu.make_async_remote_copy(
            src_ref=src,
            dst_ref=dst,
            send_sem=halo_send_sem.at[mine],
            recv_sem=halo_recv_sem.at[theirs],
            device_id=device,
            device_id_type=MESH,
        )

    x_copies = []
    for side, x in enumerate((gx_lo, gx_hi)):
        copies = [
            remote(c_send.at[side, ys], c_recv.at[1 - side, 1 - ys], 3 + side, 4 - side, (x, y))
            for ys, y in enumerate((gy_lo, gy_hi))
        ]
        copies.append(remote(x_send.at[side], x_recv.at[1 - side], 1 + side, 2 - side, (x, gy)))
        x_copies.append(copies)

        @pl.when(has_x[side])
        def _():
            for copy in copies[:2]:
                copy.start()

    remote(y_send.at[0], y_recv.at[1], 0, 0, (gx, gy_lo)).start()
    remote(y_send.at[1], y_recv.at[0], 0, 0, (gx, gy_hi)).start()
    for side in range(2):

        @pl.when(has_x[side])
        def _():
            x_copies[side][2].start()

    for copy in params[2:]:
        copy.wait()

    x_open = (jnp.logical_or(row > 0, has_x[0]), jnp.logical_or(row < SIDE - 1, has_x[1]))
    y_open = (jnp.logical_or(row > 0, has_y[0]), jnp.logical_or(row < SIDE - 1, has_y[1]))

    own_vertical = [vertical(head[y], temp[y], conduct[y], lane) for y in range(SIDE)]

    whole_y = remote(y_send, y_recv, 0, 0, (gx, gy_lo))
    whole_x = [
        (
            remote(x_send.at[side], x_recv.at[side], 1 + side, 1 + side, (gx, gy_lo)),
            remote(c_send.at[side], c_recv.at[side], 3 + side, 3 + side, (gx, gy_lo)),
        )
        for side in range(2)
    ]
    whole_y.wait_recv()
    for side in range(2):

        @pl.when(has_x[side])
        def _():
            for copy in whole_x[side]:
                copy.wait_recv()

    def along_rows(value, before, after):
        return (
            jnp.where(first, before, pltpu.roll(value, 1, 0)),
            jnp.where(last, after, pltpu.roll(value, SIDE - 1, 0)),
        )

    def change_rows(head_, conduct_, temp_, ends, opened):
        (h_lo, t_lo, k_lo), (h_hi, t_hi, k_hi) = ends
        heads = along_rows(head_, h_lo, h_hi)
        temps = along_rows(temp_, t_lo, t_hi)
        conducts = along_rows(conduct_, k_lo, k_hi)
        total = sum(
            jnp.where(opened[s], (conduct_ + conducts[s]) * (heads[s] - head_), 0.0)
            for s in range(2)
        )
        return total, temps[0] + temps[1]

    def y_part(side, number):
        return y_recv[side, pl.ds(number * SIDE, SIDE), :]

    def x_part(side, number):
        return x_recv[side, pl.ds(number * SIDE, SIDE), :]

    def warm_if(present, value):
        return jnp.where(present, value, 0.0)

    def corner(xs, ys):
        return (
            c_recv[xs, ys, pl.ds(0, 1), :],
            warm_if(jnp.logical_and(has_x[xs], has_y[ys]), c_recv[xs, ys, pl.ds(1, 1), :]),
            c_recv[xs, ys, pl.ds(2, 1), :],
        )

    y_ghost, x_ghost = [], []
    for part_of, present, dest in ((y_part, has_y, y_ghost), (x_part, has_x, x_ghost)):
        for side in range(2):
            h, t, c, i = (part_of(side, number) for number in range(4))
            k_s, a = lookup(c, ks_s), lookup(c, alpha_s)
            k = conductivity(h, t, k_s, a, i)
            far = tuple(part_of(side, number) for number in range(4, 7))
            dest.append((h, warm_if(present[side], t), k, k_s, a, i, far))

    for side in range(2):
        for field in range(3):
            ghost[side, field] = x_ghost[side][field]

    def step(h, t, change, warm):
        return h + 0.5 * change, t + DIFFUSE * (warm - 6.0 * t)

    def face(k_a, h_a, k_b, h_b):
        return (k_a + k_b) * (h_b - h_a)

    def ghost_step(cell, inner, ends, opened, present):
        h, t, k, k_s, a, i, far = cell
        change, warm = vertical(h, t, k, lane)
        rows, rows_warm = change_rows(h, k, t, ends, opened)
        change = change + rows + face(k, h, far[2], far[0]) + face(k, h, inner[2], inner[0])
        warm = warm + rows_warm + far[1] + inner[1]
        h, t = step(h, t, change, warm)
        return h, warm_if(present, t), conductivity(h, t, k_s, a, i)

    y_next = [
        ghost_step(
            y_ghost[side],
            (head[y], temp[y], conduct[y]),
            (corner(0, side), corner(1, side)),
            x_open,
            has_y[side],
        )
        for side, y in ((0, 0), (1, SIDE - 1))
    ]
    x_next = [
        ghost_step(
            x_ghost[side],
            (edge[x][0], edge[x][1], edge[x][4]),
            (corner(side, 0), corner(side, 1)),
            y_open,
            has_x[side],
        )
        for side, x in ((0, 0), (1, SIDE - 1))
    ]
    for side in range(2):
        for field in range(3):
            ghost[2 + side, field] = x_next[side][field]

    def main_step(head_, temp_, conduct_, lows, highs, slot, verticals):
        hs = [lows[0], *head_, highs[0]]
        ts = [lows[1], *temp_, highs[1]]
        ks_ = [lows[2], *conduct_, highs[2]]
        faces = [face(ks_[y], hs[y], ks_[y + 1], hs[y + 1]) for y in range(SIDE + 1)]
        faces[0] = jnp.where(has_y[0], faces[0], 0.0)
        faces[SIDE] = jnp.where(has_y[1], faces[SIDE], 0.0)
        result = []
        for y in range(SIDE):
            ends = tuple(
                tuple(ghost[slot + side, field, pl.ds(y, 1), :] for field in range(3))
                for side in range(2)
            )
            rows, rows_warm = change_rows(head_[y], conduct_[y], temp_[y], ends, x_open)
            change, warm = verticals[y]
            change = change + rows + faces[y + 1] - faces[y]
            warm = warm + rows_warm + ts[y] + ts[y + 2]
            result.append(step(head_[y], temp_[y], change, warm))
        return [r[0] for r in result], [r[1] for r in result]

    head, temp = main_step(head, temp, conduct, y_ghost[0], y_ghost[1], 0, own_vertical)
    conduct = [
        conductivity(head[y], temp[y], ks[y], alpha[y], ice[y]) for y in range(SIDE)
    ]
    verticals = [vertical(head[y], temp[y], conduct[y], lane) for y in range(SIDE)]
    head, temp = main_step(head, temp, conduct, y_next[0], y_next[1], 2, verticals)

    for y in range(SIDE):
        head_v[pl.ds(y, SIDE, stride=SIDE), :] = head[y]
        temp_v[pl.ds(y, SIDE, stride=SIDE), :] = temp[y]

    theta = [0.05 + 0.4 * jnp.exp(0.8 * jnp.minimum(h, 0.0)) for h in head]
    planes_all = gy_count * SIDE
    layers = []
    for view in range(VIEWS):
        clear = None
        sums = [None] * 3
        depth = None
        for y in range(SIDE):
            shift = skew_s[view] * ((gy * SIDE + y).astype(F32) - 0.5 * planes_all)
            wrapped = shift - DEPTH * jnp.floor(shift * (1.0 / DEPTH))
            base = jnp.floor(wrapped)
            part = wrapped - base
            turn = lax.rem(2 * DEPTH - base.astype(jnp.int32), DEPTH)
            lower = pltpu.roll(theta[y], turn, 1)
            upper = pltpu.roll(lower, DEPTH - 1, 1)
            sample = (1.0 - part) * lower + part * upper
            optical = sample * (8.0 / planes_all)
            passed = jnp.exp(-optical)
            after = passed if clear is None else clear * passed
            weight = (1.0 if clear is None else clear) - after
            clear = after
            depth = optical if depth is None else depth + optical
            for color in range(3):
                term = weight * jnp.tanh((0.5 * steep_s[color]) * (sample - mid_s[color]))
                sums[color] = term if sums[color] is None else sums[color] + term
        layers += [0.5 * ((1.0 - clear) + total) for total in sums]
        layers.append(depth)
    piece_send[...] = jnp.transpose(jnp.concatenate(layers, 0))

    def exchange(src, dst, device):
        return pltpu.make_async_remote_copy(
            src_ref=src,
            dst_ref=dst,
            send_sem=piece_send_sem,
            recv_sem=piece_recv_sem,
            device_id=device,
            device_id_type=MESH,
        )

    for peer in peers:
        exchange(
            piece_send.at[pl.ds(pl.multiple_of(peer * SIDE, SIDE), SIDE)],
            piece_recv.at[gy],
            (gx, peer),
        ).start()
    piece_recv[gy] = piece_send[pl.ds(pl.multiple_of(gy * SIDE, SIDE), SIDE), :]

    view_of = lax.div(lane, 4 * SIDE)
    kind_of = lax.rem(lax.div(lane, SIDE), 4)
    ranks = []
    for group in range(GROUPS):
        rank = jnp.full((SIDE, DEPTH), order_s[0, group], jnp.int32)
        for view in range(1, VIEWS):
            rank = jnp.where(view_of == view, order_s[view, group], rank)
        ranks.append(rank)
    is_depth = kind_of == 3

    exchange_in = pltpu.make_async_remote_copy(
        src_ref=piece_recv.at[pl.ds(0, GROUPS - 1)],
        dst_ref=piece_recv.at[pl.ds(0, GROUPS - 1)],
        send_sem=piece_send_sem,
        recv_sem=piece_recv_sem,
        device_id=(gx, gy_lo),
        device_id_type=MESH,
    )
    exchange_in.wait_recv()

    depths = []
    for group in range(GROUPS):
        value = jnp.where(is_depth, piece_recv[group], 0.0)
        value = value + pltpu.roll(value, DEPTH - SIDE, 1)
        depths.append(value + pltpu.roll(value, DEPTH - 2 * SIDE, 1))
    fronts = [jnp.zeros((SIDE, DEPTH), F32)] * GROUPS
    for one in range(GROUPS):
        for two in range(one + 1, GROUPS):
            before = ranks[two] < ranks[one]
            fronts[one] = fronts[one] + jnp.where(before, depths[two], 0.0)
            fronts[two] = fronts[two] + jnp.where(before, 0.0, depths[one])
    color = sum(jnp.exp(-fronts[group]) * piece_recv[group] for group in range(GROUPS))
    opaque = 1.0 - jnp.exp(-sum(depths))
    image_v[...] = jnp.transpose(jnp.where(is_depth, opaque, color))
    whole_y.wait_send()
    for side in range(2):

        @pl.when(has_x[side])
        def _():
            for copy in whole_x[side]:
                copy.wait_send()

    exchange_in.wait_send()


def put_out(head_v, temp_v, image_v, head_out, temp_out, image_out, sem):
    copies = [
        pltpu.make_async_copy(src, dst, sem.at[number])
        for number, (src, dst) in enumerate(
            ((image_v, image_out), (head_v, head_out), (temp_v, temp_out))
        )
    ]
    for copy in copies:
        copy.start()
    for copy in copies:
        copy.wait()


def shards(head, temp, category, ice, *params):
    gx_count, gy_count = lax.axis_size("gx"), lax.axis_size("gy")
    rows = SIDE * SIDE
    flat = [a.reshape(rows, DEPTH) for a in (head, temp, category, ice)]
    vmem = pltpu.VMEM
    dma = pltpu.SemaphoreType.DMA
    shapes = ((rows, DEPTH), (rows, DEPTH), (DEPTH, SIDE))
    results = pl.pallas_call(
        functools.partial(kernel, gx_count, gy_count),
        out_shape=tuple(pltpu.VMEM(shape, F32) for shape in shapes),
        in_specs=[pl.BlockSpec(memory_space=pl.ANY)] * 10,
        out_specs=[pl.BlockSpec(memory_space=pltpu.VMEM)] * 3,
        scratch_shapes=[
            vmem((rows, DEPTH), F32),
            vmem((rows, DEPTH), F32),
            vmem((rows, DEPTH), jnp.int32),
            vmem((rows, DEPTH), jnp.int32),
            pltpu.SMEM((SOILS,), F32),
            pltpu.SMEM((SOILS,), F32),
            pltpu.SMEM((VIEWS,), F32),
            pltpu.SMEM((3,), F32),
            pltpu.SMEM((3,), F32),
            pltpu.SMEM((VIEWS, GROUPS), jnp.int32),
            vmem((2, 7 * SIDE, DEPTH), F32),
            vmem((2, 7 * SIDE, DEPTH), F32),
            vmem((2, 7 * SIDE, DEPTH), F32),
            vmem((2, 7 * SIDE, DEPTH), F32),
            vmem((2, 2, 4, DEPTH), F32),
            vmem((2, 2, 4, DEPTH), F32),
            vmem((4, 3, SIDE, DEPTH), F32),
            vmem((DEPTH, DEPTH), F32),
            vmem((GROUPS, SIDE, DEPTH), F32),
            dma((4,)),
            dma((6,)),
            dma((5,)),
            dma((5,)),
            dma(()),
            dma(()),
        ],
        compiler_params=pltpu.CompilerParams(collective_id=0, has_side_effects=True),
        name="step_and_view",
    )(*flat, *params)
    head, temp, image = pl.pallas_call(
        put_out,
        out_shape=tuple(jax.ShapeDtypeStruct(shape, F32) for shape in shapes),
        in_specs=[pl.BlockSpec(memory_space=pltpu.VMEM)] * 3,
        out_specs=[pl.BlockSpec(memory_space=pl.ANY)] * 3,
        scratch_shapes=[dma((3,))],
        name="put_out",
    )(*(pltpu.with_memory_space_constraint(r, pltpu.VMEM) for r in results))
    shape = (SIDE, SIDE, DEPTH)
    return head.reshape(shape), temp.reshape(shape), image.reshape(VIEWS, 4, SIDE, SIDE)


def solution(mesh):
    block = P("gx", "gy", None)
    return jax.shard_map(
        shards,
        mesh=mesh,
        in_specs=(block,) * 4 + (P(),) * 6,
        out_specs=(block, block, P(None, None, "gx", "gy")),
        check_vma=False,
    )
```

```python
import functools

import jax
import jax.numpy as jnp
from jax import lax
from jax.experimental import pallas as pl
from jax.experimental.pallas import tpu as pltpu
from jax.sharding import PartitionSpec as P

MESH = pl.DeviceIdType.MESH
SOILS = 12
VIEWS = 4
SIDE = 8
DEPTH = 128
GROUPS = 16
DIFFUSE = 0.12
F32 = jnp.float32


def lookup(category, table):
    total = jnp.full(category.shape, table[0], F32)
    for number in range(1, SOILS):
        total = jnp.where(category == number, table[number], total)
    return total


def conductivity(head, temp, ks, alpha, ice):
    return ks * jnp.exp(alpha * jnp.minimum(head, 0.0) + 2.0 * ice * (jnp.tanh(temp) - 1.0))


def vertical(head, temp, conduct, lane):
    above = pltpu.roll(head, DEPTH - 1, 1)
    conduct_above = pltpu.roll(conduct, DEPTH - 1, 1)
    flux = jnp.where(lane < DEPTH - 1, (conduct + conduct_above) * (above - head + 1.0), 0.0)
    change = flux - pltpu.roll(flux, 1, 1)
    warm = jnp.where(lane < DEPTH - 1, pltpu.roll(temp, DEPTH - 1, 1), 0.0) + jnp.where(
        lane > 0, pltpu.roll(temp, 1, 1), 0.0
    )
    return change, warm


def kernel(
    gx_count,
    gy_count,
    head_in,
    temp_in,
    cat_in,
    ice_in,
    ks_in,
    alpha_in,
    skew_in,
    steep_in,
    mid_in,
    order_in,
    head_v,
    temp_v,
    image_v,
    head_a,
    temp_a,
    cat_a,
    ice_a,
    ks_s,
    alpha_s,
    skew_s,
    steep_s,
    mid_s,
    order_s,
    y_send,
    y_recv,
    x_send,
    x_recv,
    c_send,
    c_recv,
    ghost,
    piece_send,
    piece_recv,
    in_sem,
    par_sem,
    halo_send_sem,
    halo_recv_sem,
    known_sem,
    piece_send_sem,
    piece_recv_sem,
):
    gx, gy = lax.axis_index("gx"), lax.axis_index("gy")
    gx_lo, gx_hi = lax.rem(gx + gx_count - 1, gx_count), lax.rem(gx + 1, gx_count)
    gy_lo, gy_hi = lax.rem(gy + gy_count - 1, gy_count), lax.rem(gy + 1, gy_count)

    loads = [
        pltpu.make_async_copy(src, dst, in_sem.at[number])
        for number, (src, dst) in enumerate(
            ((head_in, head_a), (temp_in, temp_a), (cat_in, cat_a), (ice_in, ice_a))
        )
    ]
    params = [
        pltpu.make_async_copy(src, dst, par_sem.at[number])
        for number, (src, dst) in enumerate(
            (
                (ks_in, ks_s),
                (alpha_in, alpha_s),
                (skew_in, skew_s),
                (steep_in, steep_s),
                (mid_in, mid_s),
                (order_in, order_s),
            )
        )
    ]
    for copy in params[:2] + loads + params[2:]:
        copy.start()

    px, py = lax.div(gy, 4), lax.rem(gy, 4)
    shifts = sorted(
        ((dx, dy) for dx in range(4) for dy in range(4) if (dx, dy) != (0, 0)),
        key=lambda d: -(min(d[0], 4 - d[0]) + min(d[1], 4 - d[1])),
    )
    peers = [lax.rem(px + dx, 4) * 4 + lax.rem(py + dy, 4) for dx, dy in shifts]

    has_x = (gx > 0, gx < gx_count - 1)
    has_y = (gy > 0, gy < gy_count - 1)
    x_at, y_at = (gx_lo, gx_hi), (gy_lo, gy_hi)
    both = [[jnp.logical_and(has_x[a], has_y[b]) for b in range(2)] for a in range(2)]
    hub = 1 + lax.rem(gx, 2)
    is_hub = gy == hub
    far_from_hub = jnp.abs(gy - hub) > 1

    barrier = pltpu.get_barrier_semaphore()

    def greet(device):
        pl.semaphore_signal(barrier, inc=1, device_id=device, device_id_type=MESH)

    for a in range(2):
        for b in range(2):

            @pl.when(both[a][b])
            def _():
                greet((x_at[a], y_at[b]))

    for b in range(2):

        @pl.when(has_y[b])
        def _():
            greet((gx, y_at[b]))

    @pl.when(far_from_hub)
    def _():
        greet((gx, hub))

    for a in range(2):

        @pl.when(has_x[a])
        def _():
            greet((x_at[a], gy))

    row = lax.broadcasted_iota(jnp.int32, (SIDE, DEPTH), 0)
    lane = lax.broadcasted_iota(jnp.int32, (SIDE, DEPTH), 1)
    first, last = row == 0, row == SIDE - 1

    for copy in params[:2]:
        copy.wait()
    for copy in loads:
        copy.wait()

    def across(ref, y):
        return ref[pl.ds(y, SIDE, stride=SIDE), :]

    def tile(ref, x):
        return ref[pl.ds(x * SIDE, SIDE), :]

    head = [across(head_a, y) for y in range(SIDE)]
    temp = [across(temp_a, y) for y in range(SIDE)]
    category = [across(cat_a, y) for y in range(SIDE)]
    ice = [across(ice_a, y).astype(F32) for y in range(SIDE)]
    ks = [lookup(category[y], ks_s) for y in range(SIDE)]
    alpha = [lookup(category[y], alpha_s) for y in range(SIDE)]
    conduct = [
        conductivity(head[y], temp[y], ks[y], alpha[y], ice[y]) for y in range(SIDE)
    ]
    edge = {}
    for x in (0, 1, SIDE - 2, SIDE - 1):
        h, t, c = tile(head_a, x), tile(temp_a, x), tile(cat_a, x)
        i = tile(ice_a, x).astype(F32)
        k = conductivity(h, t, lookup(c, ks_s), lookup(c, alpha_s), i)
        edge[x] = (h, t, c.astype(F32), i, k)

    for side, (near, far) in enumerate(((0, 1), (SIDE - 1, SIDE - 2))):
        parts = (
            head[near],
            temp[near],
            category[near].astype(F32),
            ice[near],
            head[far],
            temp[far],
            conduct[far],
        )
        for number, part in enumerate(parts):
            y_send[side, pl.ds(number * SIDE, SIDE), :] = part
        parts = (*edge[near][:4], edge[far][0], edge[far][1], edge[far][4])
        for number, part in enumerate(parts):
            x_send[side, pl.ds(number * SIDE, SIDE), :] = part
    for number, (x, y) in enumerate(((0, 0), (0, 7), (7, 0), (7, 7))):
        for field, part in enumerate((head[y], temp[y], conduct[y], conduct[y])):
            c_send[number // 2, number % 2, pl.ds(field, 1), :] = part[x : x + 1, :]

    def count(flags):
        return sum(flag.astype(jnp.int32) for flag in flags)

    x_sides, y_sides = count(has_x), count(has_y)
    gathered = jnp.where(is_hub, gy_count - 3, 0)
    pl.semaphore_wait(barrier, gathered + y_sides + x_sides * (1 + y_sides))

    def remote(src, dst, mine, theirs, device):
        return pltpu.make_async_remote_copy(
            src_ref=src,
            dst_ref=dst,
            send_sem=halo_send_sem.at[mine],
            recv_sem=halo_recv_sem.at[theirs],
            device_id=device,
            device_id_type=MESH,
        )

    def y_copy(b):
        return remote(y_send.at[b], y_recv.at[1 - b], b, 1 - b, (gx, y_at[b]))

    def x_copy(a):
        return remote(x_send.at[a], x_recv.at[1 - a], 2 + a, 3 - a, (x_at[a], gy))

    def c_copy(a, b):
        slot = 4 + 2 * a + b
        return remote(
            c_send.at[a, b], c_recv.at[1 - a, 1 - b], slot, 11 - slot, (x_at[a], y_at[b])
        )

    copies = [(both[a][b], c_copy(a, b)) for a in range(2) for b in range(2)]
    copies += [(has_y[b], y_copy(b)) for b in range(2)]
    copies += [(has_x[a], x_copy(a)) for a in range(2)]
    for present, copy in copies:

        @pl.when(present)
        def _():
            copy.start()

    @pl.when(is_hub)
    def _():
        for peer in peers:
            pl.semaphore_signal(known_sem, inc=1, device_id=(gx, peer), device_id_type=MESH)

    for copy in params[2:]:
        copy.wait()

    x_open = (jnp.logical_or(row > 0, has_x[0]), jnp.logical_or(row < SIDE - 1, has_x[1]))
    y_open = (jnp.logical_or(row > 0, has_y[0]), jnp.logical_or(row < SIDE - 1, has_y[1]))

    own_vertical = [vertical(head[y], temp[y], conduct[y], lane) for y in range(SIDE)]

    def arrived(a, b):
        slot = 4 + 2 * a + b
        return remote(c_send.at[a, b], c_recv.at[a, b], slot, slot, (gx, gy_lo))

    waits = [(has_x[a], remote(x_send.at[a], x_recv.at[a], 2 + a, 2 + a, (gx, gy_lo))) for a in range(2)]
    waits += [(both[a][b], arrived(a, b)) for a in range(2) for b in range(2)]
    waits += [(has_y[b], remote(y_send.at[b], y_recv.at[b], b, b, (gx, gy_lo))) for b in range(2)]
    for present, copy in waits:

        @pl.when(present)
        def _():
            copy.wait_recv()

    def along_rows(value, before, after):
        return (
            jnp.where(first, before, pltpu.roll(value, 1, 0)),
            jnp.where(last, after, pltpu.roll(value, SIDE - 1, 0)),
        )

    def change_rows(head_, conduct_, temp_, ends, opened):
        (h_lo, t_lo, k_lo), (h_hi, t_hi, k_hi) = ends
        heads = along_rows(head_, h_lo, h_hi)
        temps = along_rows(temp_, t_lo, t_hi)
        conducts = along_rows(conduct_, k_lo, k_hi)
        total = sum(
            jnp.where(opened[s], (conduct_ + conducts[s]) * (heads[s] - head_), 0.0)
            for s in range(2)
        )
        return total, temps[0] + temps[1]

    def y_part(side, number):
        return y_recv[side, pl.ds(number * SIDE, SIDE), :]

    def x_part(side, number):
        return x_recv[side, pl.ds(number * SIDE, SIDE), :]

    def warm_if(present, value):
        return jnp.where(present, value, 0.0)

    def corner(xs, ys):
        return (
            c_recv[xs, ys, pl.ds(0, 1), :],
            warm_if(jnp.logical_and(has_x[xs], has_y[ys]), c_recv[xs, ys, pl.ds(1, 1), :]),
            c_recv[xs, ys, pl.ds(2, 1), :],
        )

    y_ghost, x_ghost = [], []
    for part_of, present, dest in ((y_part, has_y, y_ghost), (x_part, has_x, x_ghost)):
        for side in range(2):
            h, t, c, i = (part_of(side, number) for number in range(4))
            k_s, a = lookup(c, ks_s), lookup(c, alpha_s)
            k = conductivity(h, t, k_s, a, i)
            far = tuple(part_of(side, number) for number in range(4, 7))
            dest.append((h, warm_if(present[side], t), k, k_s, a, i, far))

    for side in range(2):
        for field in range(3):
            ghost[side, field] = x_ghost[side][field]

    def step(h, t, change, warm):
        return h + 0.5 * change, t + DIFFUSE * (warm - 6.0 * t)

    def face(k_a, h_a, k_b, h_b):
        return (k_a + k_b) * (h_b - h_a)

    def ghost_step(cell, inner, ends, opened, present):
        h, t, k, k_s, a, i, far = cell
        change, warm = vertical(h, t, k, lane)
        rows, rows_warm = change_rows(h, k, t, ends, opened)
        change = change + rows + face(k, h, far[2], far[0]) + face(k, h, inner[2], inner[0])
        warm = warm + rows_warm + far[1] + inner[1]
        h, t = step(h, t, change, warm)
        return h, warm_if(present, t), conductivity(h, t, k_s, a, i)

    y_next = [
        ghost_step(
            y_ghost[side],
            (head[y], temp[y], conduct[y]),
            (corner(0, side), corner(1, side)),
            x_open,
            has_y[side],
        )
        for side, y in ((0, 0), (1, SIDE - 1))
    ]
    x_next = [
        ghost_step(
            x_ghost[side],
            (edge[x][0], edge[x][1], edge[x][4]),
            (corner(side, 0), corner(side, 1)),
            y_open,
            has_x[side],
        )
        for side, x in ((0, 0), (1, SIDE - 1))
    ]
    for side in range(2):
        for field in range(3):
            ghost[2 + side, field] = x_next[side][field]

    def main_step(head_, temp_, conduct_, lows, highs, slot, verticals):
        hs = [lows[0], *head_, highs[0]]
        ts = [lows[1], *temp_, highs[1]]
        ks_ = [lows[2], *conduct_, highs[2]]
        faces = [face(ks_[y], hs[y], ks_[y + 1], hs[y + 1]) for y in range(SIDE + 1)]
        faces[0] = jnp.where(has_y[0], faces[0], 0.0)
        faces[SIDE] = jnp.where(has_y[1], faces[SIDE], 0.0)
        result = []
        for y in range(SIDE):
            ends = tuple(
                tuple(ghost[slot + side, field, pl.ds(y, 1), :] for field in range(3))
                for side in range(2)
            )
            rows, rows_warm = change_rows(head_[y], conduct_[y], temp_[y], ends, x_open)
            change, warm = verticals[y]
            change = change + rows + faces[y + 1] - faces[y]
            warm = warm + rows_warm + ts[y] + ts[y + 2]
            result.append(step(head_[y], temp_[y], change, warm))
        return [r[0] for r in result], [r[1] for r in result]

    head, temp = main_step(head, temp, conduct, y_ghost[0], y_ghost[1], 0, own_vertical)
    conduct = [
        conductivity(head[y], temp[y], ks[y], alpha[y], ice[y]) for y in range(SIDE)
    ]
    verticals = [vertical(head[y], temp[y], conduct[y], lane) for y in range(SIDE)]
    head, temp = main_step(head, temp, conduct, y_next[0], y_next[1], 2, verticals)

    for y in range(SIDE):
        head_v[pl.ds(y, SIDE, stride=SIDE), :] = head[y]
        temp_v[pl.ds(y, SIDE, stride=SIDE), :] = temp[y]

    theta = [0.05 + 0.4 * jnp.exp(0.8 * jnp.minimum(h, 0.0)) for h in head]
    planes_all = gy_count * SIDE
    layers = []
    for view in range(VIEWS):
        clear = None
        sums = [None] * 3
        depth = None
        for y in range(SIDE):
            shift = skew_s[view] * ((gy * SIDE + y).astype(F32) - 0.5 * planes_all)
            wrapped = shift - DEPTH * jnp.floor(shift * (1.0 / DEPTH))
            base = jnp.floor(wrapped)
            part = wrapped - base
            turn = lax.rem(2 * DEPTH - base.astype(jnp.int32), DEPTH)
            lower = pltpu.roll(theta[y], turn, 1)
            upper = pltpu.roll(lower, DEPTH - 1, 1)
            sample = (1.0 - part) * lower + part * upper
            optical = sample * (8.0 / planes_all)
            passed = jnp.exp(-optical)
            after = passed if clear is None else clear * passed
            weight = (1.0 if clear is None else clear) - after
            clear = after
            depth = optical if depth is None else depth + optical
            for color in range(3):
                term = weight * jnp.tanh((0.5 * steep_s[color]) * (sample - mid_s[color]))
                sums[color] = term if sums[color] is None else sums[color] + term
        layers += [0.5 * ((1.0 - clear) + total) for total in sums]
        layers.append(depth)
    piece_send[...] = jnp.transpose(jnp.concatenate(layers, 0))

    def exchange(src, dst, device):
        return pltpu.make_async_remote_copy(
            src_ref=src,
            dst_ref=dst,
            send_sem=piece_send_sem,
            recv_sem=piece_recv_sem,
            device_id=device,
            device_id_type=MESH,
        )

    @pl.when(jnp.logical_not(is_hub))
    def _():
        pl.semaphore_wait(known_sem, 1)

    for peer in peers:
        exchange(
            piece_send.at[pl.ds(pl.multiple_of(peer * SIDE, SIDE), SIDE)],
            piece_recv.at[gy],
            (gx, peer),
        ).start()
    piece_recv[gy] = piece_send[pl.ds(pl.multiple_of(gy * SIDE, SIDE), SIDE), :]

    view_of = lax.div(lane, 4 * SIDE)
    kind_of = lax.rem(lax.div(lane, SIDE), 4)
    ranks = []
    for group in range(GROUPS):
        rank = jnp.full((SIDE, DEPTH), order_s[0, group], jnp.int32)
        for view in range(1, VIEWS):
            rank = jnp.where(view_of == view, order_s[view, group], rank)
        ranks.append(rank)
    is_depth = kind_of == 3

    exchange_in = pltpu.make_async_remote_copy(
        src_ref=piece_recv.at[pl.ds(0, GROUPS - 1)],
        dst_ref=piece_recv.at[pl.ds(0, GROUPS - 1)],
        send_sem=piece_send_sem,
        recv_sem=piece_recv_sem,
        device_id=(gx, gy_lo),
        device_id_type=MESH,
    )
    exchange_in.wait_recv()

    depths = []
    for group in range(GROUPS):
        value = jnp.where(is_depth, piece_recv[group], 0.0)
        value = value + pltpu.roll(value, DEPTH - SIDE, 1)
        depths.append(value + pltpu.roll(value, DEPTH - 2 * SIDE, 1))
    fronts = [jnp.zeros((SIDE, DEPTH), F32)] * GROUPS
    for one in range(GROUPS):
        for two in range(one + 1, GROUPS):
            before = ranks[two] < ranks[one]
            fronts[one] = fronts[one] + jnp.where(before, depths[two], 0.0)
            fronts[two] = fronts[two] + jnp.where(before, 0.0, depths[one])
    color = sum(jnp.exp(-fronts[group]) * piece_recv[group] for group in range(GROUPS))
    opaque = 1.0 - jnp.exp(-sum(depths))
    image_v[...] = jnp.transpose(jnp.where(is_depth, opaque, color))
    for present, copy in waits:

        @pl.when(present)
        def _():
            copy.wait_send()

    exchange_in.wait_send()


def put_out(head_v, temp_v, image_v, head_out, temp_out, image_out, sem):
    copies = [
        pltpu.make_async_copy(src, dst, sem.at[number])
        for number, (src, dst) in enumerate(
            ((image_v, image_out), (head_v, head_out), (temp_v, temp_out))
        )
    ]
    for copy in copies:
        copy.start()
    for copy in copies:
        copy.wait()


def shards(head, temp, category, ice, *params):
    gx_count, gy_count = lax.axis_size("gx"), lax.axis_size("gy")
    rows = SIDE * SIDE
    flat = [a.reshape(rows, DEPTH) for a in (head, temp, category, ice)]
    vmem = pltpu.VMEM
    dma = pltpu.SemaphoreType.DMA
    shapes = ((rows, DEPTH), (rows, DEPTH), (DEPTH, SIDE))
    results = pl.pallas_call(
        functools.partial(kernel, gx_count, gy_count),
        out_shape=tuple(pltpu.VMEM(shape, F32) for shape in shapes),
        in_specs=[pl.BlockSpec(memory_space=pl.ANY)] * 10,
        out_specs=[pl.BlockSpec(memory_space=pltpu.VMEM)] * 3,
        scratch_shapes=[
            vmem((rows, DEPTH), F32),
            vmem((rows, DEPTH), F32),
            vmem((rows, DEPTH), jnp.int32),
            vmem((rows, DEPTH), jnp.int32),
            pltpu.SMEM((SOILS,), F32),
            pltpu.SMEM((SOILS,), F32),
            pltpu.SMEM((VIEWS,), F32),
            pltpu.SMEM((3,), F32),
            pltpu.SMEM((3,), F32),
            pltpu.SMEM((VIEWS, GROUPS), jnp.int32),
            vmem((2, 7 * SIDE, DEPTH), F32),
            vmem((2, 7 * SIDE, DEPTH), F32),
            vmem((2, 7 * SIDE, DEPTH), F32),
            vmem((2, 7 * SIDE, DEPTH), F32),
            vmem((2, 2, 4, DEPTH), F32),
            vmem((2, 2, 4, DEPTH), F32),
            vmem((4, 3, SIDE, DEPTH), F32),
            vmem((DEPTH, DEPTH), F32),
            vmem((GROUPS, SIDE, DEPTH), F32),
            dma((4,)),
            dma((6,)),
            dma((8,)),
            dma((8,)),
            pltpu.SemaphoreType.REGULAR(()),
            dma(()),
            dma(()),
        ],
        compiler_params=pltpu.CompilerParams(collective_id=0, has_side_effects=True),
        name="step_and_view",
    )(*flat, *params)
    head, temp, image = pl.pallas_call(
        put_out,
        out_shape=tuple(jax.ShapeDtypeStruct(shape, F32) for shape in shapes),
        in_specs=[pl.BlockSpec(memory_space=pltpu.VMEM)] * 3,
        out_specs=[pl.BlockSpec(memory_space=pl.ANY)] * 3,
        scratch_shapes=[dma((3,))],
        name="put_out",
    )(*(pltpu.with_memory_space_constraint(r, pltpu.VMEM) for r in results))
    shape = (SIDE, SIDE, DEPTH)
    return head.reshape(shape), temp.reshape(shape), image.reshape(VIEWS, 4, SIDE, SIDE)


def solution(mesh):
    block = P("gx", "gy", None)
    return jax.shard_map(
        shards,
        mesh=mesh,
        in_specs=(block,) * 4 + (P(),) * 6,
        out_specs=(block, block, P(None, None, "gx", "gy")),
        check_vma=False,
    )
```

```python
import functools

import jax
import jax.numpy as jnp
from jax import lax
from jax.experimental import pallas as pl
from jax.experimental.pallas import tpu as pltpu
from jax.sharding import PartitionSpec as P

MESH = pl.DeviceIdType.MESH
SOILS = 12
VIEWS = 4
SIDE = 8
DEPTH = 128
GROUPS = 16
DIFFUSE = 0.12
HUB = 1
BEFORE, CROSS, BELOW, DIAGONAL, MOST, ALL = range(6)
F32 = jnp.float32


def lookup(category, table):
    total = jnp.full(category.shape, table[0], F32)
    for number in range(1, SOILS):
        total = jnp.where(category == number, table[number], total)
    return total


def conductivity(head, temp, ks, alpha, ice):
    return ks * jnp.exp(alpha * jnp.minimum(head, 0.0) + 2.0 * ice * (jnp.tanh(temp) - 1.0))


def vertical(head, temp, conduct, lane):
    above = pltpu.roll(head, DEPTH - 1, 1)
    conduct_above = pltpu.roll(conduct, DEPTH - 1, 1)
    flux = jnp.where(lane < DEPTH - 1, (conduct + conduct_above) * (above - head + 1.0), 0.0)
    change = flux - pltpu.roll(flux, 1, 1)
    warm = jnp.where(lane < DEPTH - 1, pltpu.roll(temp, DEPTH - 1, 1), 0.0) + jnp.where(
        lane > 0, pltpu.roll(temp, 1, 1), 0.0
    )
    return change, warm


def kernel(
    gx_count,
    gy_count,
    head_in,
    temp_in,
    cat_in,
    ice_in,
    ks_in,
    alpha_in,
    skew_in,
    steep_in,
    mid_in,
    order_in,
    head_v,
    temp_v,
    image_v,
    head_a,
    temp_a,
    cat_a,
    ice_a,
    ks_s,
    alpha_s,
    skew_s,
    steep_s,
    mid_s,
    order_s,
    y_send,
    y_recv,
    x_send,
    x_recv,
    c_send,
    c_recv,
    ghost,
    piece_send,
    piece_recv,
    local_sem,
    halo_recv_sem,
    known_sem,
    piece_recv_sem,
):
    gx, gy = lax.axis_index("gx"), lax.axis_index("gy")
    gx_lo, gx_hi = lax.rem(gx + gx_count - 1, gx_count), lax.rem(gx + 1, gx_count)
    gy_lo, gy_hi = lax.rem(gy + gy_count - 1, gy_count), lax.rem(gy + 1, gy_count)

    loads = [
        pltpu.make_async_copy(src, dst, local_sem.at[number])
        for number, (src, dst) in enumerate(
            ((head_in, head_a), (temp_in, temp_a), (cat_in, cat_a), (ice_in, ice_a))
        )
    ]
    params = [
        pltpu.make_async_copy(src, dst, local_sem.at[4 + number])
        for number, (src, dst) in enumerate(
            (
                (ks_in, ks_s),
                (alpha_in, alpha_s),
                (skew_in, skew_s),
                (steep_in, steep_s),
                (mid_in, mid_s),
                (order_in, order_s),
            )
        )
    ]
    for copy in params[:2] + loads + params[2:]:
        copy.start()

    px, py = lax.div(gy, 4), lax.rem(gy, 4)
    shifts = sorted(
        ((dx, dy) for dx in range(4) for dy in range(4) if (dx, dy) != (0, 0)),
        key=lambda d: -(min(d[0], 4 - d[0]) + min(d[1], 4 - d[1])),
    )
    peers = [lax.rem(px + dx, 4) * 4 + lax.rem(py + dy, 4) for dx, dy in shifts]

    has_x = (gx > 0, gx < gx_count - 1)
    has_y = (gy > 0, gy < gy_count - 1)
    x_at, y_at = (gx_lo, gx_hi), (gy_lo, gy_hi)
    both = [[jnp.logical_and(has_x[a], has_y[b]) for b in range(2)] for a in range(2)]
    is_hub = gy == HUB
    is_late = gy == HUB - 1
    far_from_hub = jnp.abs(gy - HUB) > 1

    barrier = pltpu.get_barrier_semaphore()

    def greet(device):
        pl.semaphore_signal(barrier, inc=1, device_id=device, device_id_type=MESH)

    def tell(number, device):
        pl.semaphore_signal(known_sem.at[number], inc=1, device_id=device, device_id_type=MESH)

    for a in range(2):

        @pl.when(both[a][0])
        def _():
            greet((x_at[a], gy_lo))

    @pl.when(has_y[0])
    def _():
        greet((gx, gy_lo))

    @pl.when(has_x[0])
    def _():
        greet((gx_lo, gy))

    @pl.when(far_from_hub)
    def _():
        greet((gx, HUB))

    def one(flag):
        return flag.astype(jnp.int32)

    x_sides = one(has_x[0]) + one(has_x[1])
    gathered = jnp.where(is_hub, gy_count - 3, 0)
    awaited = gathered + one(has_x[1]) + one(has_y[1]) * (1 + x_sides)

    @pl.when(awaited > 0)
    def _():
        pl.semaphore_wait(barrier, awaited)

    for a in range(2):

        @pl.when(both[a][1])
        def _():
            tell((CROSS, DIAGONAL)[a], (x_at[a], gy_hi))

    @pl.when(has_y[1])
    def _():
        tell(BELOW, (gx, gy_hi))

    @pl.when(has_x[1])
    def _():
        tell(BEFORE, (gx_hi, gy))

    @pl.when(is_hub)
    def _():
        for peer in peers:

            @pl.when(peer != HUB - 1)
            def _():
                tell(MOST, (gx, peer))

    row = lax.broadcasted_iota(jnp.int32, (SIDE, DEPTH), 0)
    lane = lax.broadcasted_iota(jnp.int32, (SIDE, DEPTH), 1)
    first, last = row == 0, row == SIDE - 1

    for copy in params + loads:
        copy.wait()

    def across(ref, y):
        return ref[pl.ds(y, SIDE, stride=SIDE), :]

    def tile(ref, x):
        return ref[pl.ds(x * SIDE, SIDE), :]

    head, temp, category, ice, ks, alpha, conduct = ({} for _ in range(7))

    def own(y):
        head[y], temp[y], category[y] = across(head_a, y), across(temp_a, y), across(cat_a, y)
        ice[y] = across(ice_a, y).astype(F32)
        ks[y], alpha[y] = lookup(category[y], ks_s), lookup(category[y], alpha_s)
        conduct[y] = conductivity(head[y], temp[y], ks[y], alpha[y], ice[y])

    for y in (0, 1, SIDE - 2, SIDE - 1):
        own(y)
    edge = {}
    for x in (0, 1, SIDE - 2, SIDE - 1):
        h, t, c = tile(head_a, x), tile(temp_a, x), tile(cat_a, x)
        i = tile(ice_a, x).astype(F32)
        k = conductivity(h, t, lookup(c, ks_s), lookup(c, alpha_s), i)
        edge[x] = (h, t, c.astype(F32), i, k)

    for side, (near, far) in enumerate(((0, 1), (SIDE - 1, SIDE - 2))):
        parts = (
            head[near],
            temp[near],
            category[near].astype(F32),
            ice[near],
            head[far],
            temp[far],
            conduct[far],
        )
        for number, part in enumerate(parts):
            y_send[side, pl.ds(number * SIDE, SIDE), :] = part
        parts = (*edge[near][:4], edge[far][0], edge[far][1], edge[far][4])
        for number, part in enumerate(parts):
            x_send[side, pl.ds(number * SIDE, SIDE), :] = part
    for number, (x, y) in enumerate(((0, 0), (0, 7), (7, 0), (7, 7))):
        for field, part in enumerate((head[y], temp[y], conduct[y], conduct[y])):
            c_send[number // 2, number % 2, pl.ds(field, 1), :] = part[x : x + 1, :]

    def remote(src, dst, mine, theirs, device):
        return pltpu.make_async_remote_copy(
            src_ref=src,
            dst_ref=dst,
            send_sem=local_sem.at[mine],
            recv_sem=halo_recv_sem.at[theirs],
            device_id=device,
            device_id_type=MESH,
        )

    def y_copy(b):
        return remote(y_send.at[b], y_recv.at[1 - b], b, 1 - b, (gx, y_at[b]))

    def x_copy(a):
        return remote(x_send.at[a], x_recv.at[1 - a], 2 + a, 3 - a, (x_at[a], gy))

    def c_copy(a, b):
        slot = 4 + 2 * a + b
        return remote(
            c_send.at[a, b], c_recv.at[1 - a, 1 - b], slot, 11 - slot, (x_at[a], y_at[b])
        )

    def send(present, copy, *known):
        @pl.when(present)
        def _():
            for number in known:
                pl.semaphore_wait(known_sem.at[number], 1)
            copy.start()

    for a in range(2):
        send(both[a][1], c_copy(a, 1))
    send(has_y[1], y_copy(1))
    send(has_x[1], x_copy(1))
    send(has_x[0], x_copy(0), BEFORE)
    send(both[1][0], c_copy(1, 0), CROSS)
    send(has_y[0], y_copy(0), BELOW)

    @pl.when(is_hub)
    def _():
        for peer in peers:
            tell(ALL, (gx, peer))

    send(both[0][0], c_copy(0, 0), DIAGONAL)

    x_open = (jnp.logical_or(row > 0, has_x[0]), jnp.logical_or(row < SIDE - 1, has_x[1]))
    y_open = (jnp.logical_or(row > 0, has_y[0]), jnp.logical_or(row < SIDE - 1, has_y[1]))

    for y in range(2, SIDE - 2):
        own(y)

    def arrived(a, b):
        slot = 4 + 2 * a + b
        return remote(c_send.at[a, b], c_recv.at[a, b], slot, slot, (gx, gy_lo))

    x_waits = [
        (has_x[a], remote(x_send.at[a], x_recv.at[a], 2 + a, 2 + a, (gx, gy_lo)))
        for a in range(2)
    ]
    y_waits = [(both[a][b], arrived(a, b)) for a in range(2) for b in range(2)]
    y_waits += [
        (has_y[b], remote(y_send.at[b], y_recv.at[b], b, b, (gx, gy_lo))) for b in range(2)
    ]

    def receive(waits):
        for present, copy in waits:

            @pl.when(present)
            def _():
                copy.wait_recv()

    def along_rows(value, before, after):
        return (
            jnp.where(first, before, pltpu.roll(value, 1, 0)),
            jnp.where(last, after, pltpu.roll(value, SIDE - 1, 0)),
        )

    def change_rows(head_, conduct_, temp_, ends, opened):
        (h_lo, t_lo, k_lo), (h_hi, t_hi, k_hi) = ends
        heads = along_rows(head_, h_lo, h_hi)
        temps = along_rows(temp_, t_lo, t_hi)
        conducts = along_rows(conduct_, k_lo, k_hi)
        total = sum(
            jnp.where(opened[s], (conduct_ + conducts[s]) * (heads[s] - head_), 0.0)
            for s in range(2)
        )
        return total, temps[0] + temps[1]

    def y_part(side, number):
        return y_recv[side, pl.ds(number * SIDE, SIDE), :]

    def x_part(side, number):
        return x_recv[side, pl.ds(number * SIDE, SIDE), :]

    def warm_if(present, value):
        return jnp.where(present, value, 0.0)

    def corner(xs, ys):
        return (
            c_recv[xs, ys, pl.ds(0, 1), :],
            warm_if(jnp.logical_and(has_x[xs], has_y[ys]), c_recv[xs, ys, pl.ds(1, 1), :]),
            c_recv[xs, ys, pl.ds(2, 1), :],
        )

    def read_ghost(part_of, side, present):
        h, t, c, i = (part_of(side, number) for number in range(4))
        k_s, a = lookup(c, ks_s), lookup(c, alpha_s)
        far = tuple(part_of(side, number) for number in range(4, 7))
        return h, warm_if(present, t), conductivity(h, t, k_s, a, i), k_s, a, i, far

    def step(h, t, change, warm):
        return h + 0.5 * change, t + DIFFUSE * (warm - 6.0 * t)

    def face(k_a, h_a, k_b, h_b):
        return (k_a + k_b) * (h_b - h_a)

    def ghost_base(cell, inner):
        h, t, k, far = cell[0], cell[1], cell[2], cell[6]
        change, warm = vertical(h, t, k, lane)
        change = change + face(k, h, far[2], far[0]) + face(k, h, inner[2], inner[0])
        return change, warm + far[1] + inner[1]

    def ghost_step(cell, base, ends, opened, present):
        h, t, k, k_s, a, i, _ = cell
        rows, rows_warm = change_rows(h, k, t, ends, opened)
        h, t = step(h, t, base[0] + rows, base[1] + rows_warm)
        return h, warm_if(present, t), conductivity(h, t, k_s, a, i)

    def keep(slot, cells):
        for side in range(2):
            for field in range(3):
                ghost[slot + side, field] = cells[side][field]

    def base_of(y, h, t, k, slot):
        ends = tuple(
            tuple(ghost[slot + side, field, pl.ds(y, 1), :] for field in range(3))
            for side in range(2)
        )
        change, warm = vertical(h[y], t[y], k[y], lane)
        rows, rows_warm = change_rows(h[y], k[y], t[y], ends, x_open)
        return change + rows, warm + rows_warm

    def plane_step(y, h, t, k, base, faces):
        for edge_ in (y, y + 1):
            if edge_ not in faces:
                value = face(k[edge_ - 1], h[edge_ - 1], k[edge_], h[edge_])
                if edge_ in (0, SIDE):
                    value = jnp.where(has_y[edge_ // SIDE], value, 0.0)
                faces[edge_] = value
        return step(
            h[y],
            t[y],
            base[0] + faces[y + 1] - faces[y],
            base[1] + t[y - 1] + t[y + 1],
        )

    planes_all = gy_count * SIDE

    def view_planes(view, planes, theta):
        clear = depth = None
        sums = [None] * 3
        for y in planes:
            shift = skew_s[view] * ((gy * SIDE + y).astype(F32) - 0.5 * planes_all)
            wrapped = shift - DEPTH * jnp.floor(shift * (1.0 / DEPTH))
            base = jnp.floor(wrapped)
            part = wrapped - base
            turn = lax.rem(2 * DEPTH - base.astype(jnp.int32), DEPTH)
            lower = pltpu.roll(theta[y], turn, 1)
            upper = pltpu.roll(lower, DEPTH - 1, 1)
            sample = (1.0 - part) * lower + part * upper
            optical = sample * (8.0 / planes_all)
            passed = jnp.exp(-optical)
            after = passed if clear is None else clear * passed
            weight = (1.0 if clear is None else clear) - after
            clear = after
            depth = optical if depth is None else depth + optical
            for color in range(3):
                term = weight * jnp.tanh((0.5 * steep_s[color]) * (sample - mid_s[color]))
                sums[color] = term if sums[color] is None else sums[color] + term
        return clear, sums, depth

    theta = {}

    def finish(y, h, t):
        head_v[pl.ds(y, SIDE, stride=SIDE), :] = h
        temp_v[pl.ds(y, SIDE, stride=SIDE), :] = t
        theta[y] = 0.05 + 0.4 * jnp.exp(0.8 * jnp.minimum(h, 0.0))

    receive(x_waits)
    x_ghost = [read_ghost(x_part, side, has_x[side]) for side in range(2)]
    keep(0, x_ghost)
    bases = [base_of(y, head, temp, conduct, 0) for y in range(SIDE)]
    faces, head_1, temp_1, conduct_1 = {}, {}, {}, {}

    def first_step(y):
        head_1[y], temp_1[y] = plane_step(y, head, temp, conduct, bases[y], faces)
        conduct_1[y] = conductivity(head_1[y], temp_1[y], ks[y], alpha[y], ice[y])

    for y in range(1, SIDE - 1):
        first_step(y)
    x_bases = [
        ghost_base(x_ghost[side], (edge[x][0], edge[x][1], edge[x][4]))
        for side, x in ((0, 0), (1, SIDE - 1))
    ]
    nothing = jnp.zeros((1, DEPTH), F32)
    keep(
        2,
        [
            ghost_step(x_ghost[side], x_bases[side], ((nothing,) * 3,) * 2, y_open, has_x[side])
            for side in range(2)
        ],
    )
    bases_1 = {y: base_of(y, head_1, temp_1, conduct_1, 2) for y in range(1, SIDE - 1)}
    faces_1 = {}
    middle = range(2, SIDE - 2)
    for y in middle:
        finish(y, *plane_step(y, head_1, temp_1, conduct_1, bases_1[y], faces_1))
    middles = [view_planes(view, middle, theta) for view in range(VIEWS)]

    receive(y_waits)
    y_ghost = [read_ghost(y_part, side, has_y[side]) for side in range(2)]
    for side, y in ((0, -1), (1, SIDE)):
        head[y], temp[y], conduct[y] = y_ghost[side][:3]
    for y in (0, SIDE - 1):
        first_step(y)
    for side, y, out in ((0, 0, -1), (1, SIDE - 1, SIDE)):
        head_1[out], temp_1[out], conduct_1[out] = ghost_step(
            y_ghost[side],
            ghost_base(y_ghost[side], (head[y], temp[y], conduct[y])),
            (corner(0, side), corner(1, side)),
            x_open,
            has_y[side],
        )
    keep(
        4,
        [
            ghost_step(
                x_ghost[side],
                x_bases[side],
                (corner(side, 0), corner(side, 1)),
                y_open,
                has_x[side],
            )
            for side in range(2)
        ],
    )
    for y in (0, SIDE - 1):
        bases_1[y] = base_of(y, head_1, temp_1, conduct_1, 4)
    for y in (0, 1, SIDE - 2, SIDE - 1):
        finish(y, *plane_step(y, head_1, temp_1, conduct_1, bases_1[y], faces_1))

    layers = []
    for view in range(VIEWS):
        clear_a, sums_a, depth_a = view_planes(view, (0, 1), theta)
        clear_b, sums_b, depth_b = middles[view]
        clear_c, sums_c, depth_c = view_planes(view, (SIDE - 2, SIDE - 1), theta)
        opaque = 1.0 - clear_a * (clear_b * clear_c)
        for color in range(3):
            total = sums_a[color] + clear_a * (sums_b[color] + clear_b * sums_c[color])
            layers.append(0.5 * (opaque + total))
        layers.append(depth_a + depth_b + depth_c)
    piece_send[...] = jnp.transpose(jnp.concatenate(layers, 0))

    def exchange(src, dst, device):
        return pltpu.make_async_remote_copy(
            src_ref=src,
            dst_ref=dst,
            send_sem=local_sem.at[8],
            recv_sem=piece_recv_sem,
            device_id=device,
            device_id_type=MESH,
        )

    plain = jnp.logical_not(jnp.logical_or(is_hub, is_late))

    def give(peer):
        exchange(
            piece_send.at[pl.ds(pl.multiple_of(peer * SIDE, SIDE), SIDE)],
            piece_recv.at[gy],
            (gx, peer),
        ).start()

    @pl.when(plain)
    def _():
        pl.semaphore_wait(known_sem.at[MOST], 1)

    @pl.when(is_late)
    def _():
        pl.semaphore_wait(known_sem.at[ALL], 1)

    for peer in peers:

        @pl.when(peer != HUB - 1)
        def _():
            give(peer)

    @pl.when(plain)
    def _():
        pl.semaphore_wait(known_sem.at[ALL], 1)

    @pl.when(jnp.logical_not(is_late))
    def _():
        give(HUB - 1)

    piece_recv[gy] = piece_send[pl.ds(pl.multiple_of(gy * SIDE, SIDE), SIDE), :]

    view_of = lax.div(lane, 4 * SIDE)
    kind_of = lax.rem(lax.div(lane, SIDE), 4)
    ranks = []
    for group in range(GROUPS):
        rank = jnp.full((SIDE, DEPTH), order_s[0, group], jnp.int32)
        for view in range(1, VIEWS):
            rank = jnp.where(view_of == view, order_s[view, group], rank)
        ranks.append(rank)
    is_depth = kind_of == 3

    exchange_in = pltpu.make_async_remote_copy(
        src_ref=piece_recv.at[pl.ds(0, GROUPS - 1)],
        dst_ref=piece_recv.at[pl.ds(0, GROUPS - 1)],
        send_sem=local_sem.at[8],
        recv_sem=piece_recv_sem,
        device_id=(gx, gy_lo),
        device_id_type=MESH,
    )
    exchange_in.wait_recv()

    depths = []
    for group in range(GROUPS):
        value = jnp.where(is_depth, piece_recv[group], 0.0)
        value = value + pltpu.roll(value, DEPTH - SIDE, 1)
        depths.append(value + pltpu.roll(value, DEPTH - 2 * SIDE, 1))
    fronts = [jnp.zeros((SIDE, DEPTH), F32)] * GROUPS
    for one in range(GROUPS):
        for two in range(one + 1, GROUPS):
            before = ranks[two] < ranks[one]
            fronts[one] = fronts[one] + jnp.where(before, depths[two], 0.0)
            fronts[two] = fronts[two] + jnp.where(before, 0.0, depths[one])
    color = sum(jnp.exp(-fronts[group]) * piece_recv[group] for group in range(GROUPS))
    opaque = 1.0 - jnp.exp(-sum(depths))
    image_v[...] = jnp.transpose(jnp.where(is_depth, opaque, color))
    for present, copy in x_waits + y_waits:

        @pl.when(present)
        def _():
            copy.wait_send()

    exchange_in.wait_send()


def put_out(head_v, temp_v, image_v, head_out, temp_out, image_out, sem):
    copies = [
        pltpu.make_async_copy(src, dst, sem.at[number])
        for number, (src, dst) in enumerate(
            ((image_v, image_out), (head_v, head_out), (temp_v, temp_out))
        )
    ]
    for copy in copies:
        copy.start()
    for copy in copies:
        copy.wait()


def shards(head, temp, category, ice, *params):
    gx_count, gy_count = lax.axis_size("gx"), lax.axis_size("gy")
    rows = SIDE * SIDE
    flat = [a.reshape(rows, DEPTH) for a in (head, temp, category, ice)]
    vmem = pltpu.VMEM
    dma = pltpu.SemaphoreType.DMA
    shapes = ((rows, DEPTH), (rows, DEPTH), (DEPTH, SIDE))
    results = pl.pallas_call(
        functools.partial(kernel, gx_count, gy_count),
        out_shape=tuple(pltpu.VMEM(shape, F32) for shape in shapes),
        in_specs=[pl.BlockSpec(memory_space=pl.ANY)] * 10,
        out_specs=[pl.BlockSpec(memory_space=pltpu.VMEM)] * 3,
        scratch_shapes=[
            vmem((rows, DEPTH), F32),
            vmem((rows, DEPTH), F32),
            vmem((rows, DEPTH), jnp.int32),
            vmem((rows, DEPTH), jnp.int32),
            pltpu.SMEM((SOILS,), F32),
            pltpu.SMEM((SOILS,), F32),
            pltpu.SMEM((VIEWS,), F32),
            pltpu.SMEM((3,), F32),
            pltpu.SMEM((3,), F32),
            pltpu.SMEM((VIEWS, GROUPS), jnp.int32),
            vmem((2, 7 * SIDE, DEPTH), F32),
            vmem((2, 7 * SIDE, DEPTH), F32),
            vmem((2, 7 * SIDE, DEPTH), F32),
            vmem((2, 7 * SIDE, DEPTH), F32),
            vmem((2, 2, 4, DEPTH), F32),
            vmem((2, 2, 4, DEPTH), F32),
            vmem((6, 3, SIDE, DEPTH), F32),
            vmem((DEPTH, DEPTH), F32),
            vmem((GROUPS, SIDE, DEPTH), F32),
            dma((10,)),
            dma((8,)),
            pltpu.SemaphoreType.REGULAR((6,)),
            dma(()),
        ],
        compiler_params=pltpu.CompilerParams(collective_id=0, has_side_effects=True),
        name="step_and_view",
    )(*flat, *params)
    head, temp, image = pl.pallas_call(
        put_out,
        out_shape=tuple(jax.ShapeDtypeStruct(shape, F32) for shape in shapes),
        in_specs=[pl.BlockSpec(memory_space=pltpu.VMEM)] * 3,
        out_specs=[pl.BlockSpec(memory_space=pl.ANY)] * 3,
        scratch_shapes=[dma((3,))],
        name="put_out",
    )(*(pltpu.with_memory_space_constraint(r, pltpu.VMEM) for r in results))
    shape = (SIDE, SIDE, DEPTH)
    return head.reshape(shape), temp.reshape(shape), image.reshape(VIEWS, 4, SIDE, SIDE)


def solution(mesh):
    block = P("gx", "gy", None)
    return jax.shard_map(
        shards,
        mesh=mesh,
        in_specs=(block,) * 4 + (P(),) * 6,
        out_specs=(block, block, P(None, None, "gx", "gy")),
        check_vma=False,
    )
```

```python
import functools

import jax
import jax.numpy as jnp
from jax import lax
from jax.experimental import pallas as pl
from jax.experimental.pallas import tpu as pltpu
from jax.sharding import PartitionSpec as P

MESH = pl.DeviceIdType.MESH
SOILS = 12
VIEWS = 4
SIDE = 8
DEPTH = 128
GROUPS = 16
DIFFUSE = 0.12
HUB = 1
LATE = 2
BEFORE, CROSS, BELOW, DIAGONAL, MOST, ALL = range(6)
F32 = jnp.float32


def lookup(category, table):
    total = jnp.full(category.shape, table[0], F32)
    for number in range(1, SOILS):
        total = jnp.where(category == number, table[number], total)
    return total


def conductivity(head, temp, ks, alpha, ice):
    return ks * jnp.exp(alpha * jnp.minimum(head, 0.0) + 2.0 * ice * (jnp.tanh(temp) - 1.0))


def vertical(head, temp, conduct, lane):
    inner_lo, inner_hi = lane > 0, lane < DEPTH - 1
    above, conduct_above = (pltpu.roll(a, DEPTH - 1, 1) for a in (head, conduct))
    below, conduct_below = (pltpu.roll(a, 1, 1) for a in (head, conduct))
    change = jnp.where(inner_hi, (conduct + conduct_above) * (above - head + 1.0), 0.0) - jnp.where(
        inner_lo, (conduct + conduct_below) * (head - below + 1.0), 0.0
    )
    warm = jnp.where(inner_hi, pltpu.roll(temp, DEPTH - 1, 1), 0.0) + jnp.where(
        inner_lo, pltpu.roll(temp, 1, 1), 0.0
    )
    return change, warm


def kernel(
    gx_count,
    gy_count,
    head_in,
    temp_in,
    cat_in,
    ice_in,
    ks_in,
    alpha_in,
    skew_in,
    steep_in,
    mid_in,
    order_in,
    head_v,
    temp_v,
    image_v,
    head_a,
    temp_a,
    cat_a,
    ice_a,
    ks_s,
    alpha_s,
    skew_s,
    steep_s,
    mid_s,
    order_s,
    y_send,
    y_recv,
    x_send,
    x_recv,
    c_send,
    c_recv,
    ghost,
    piece_send,
    piece_recv,
    local_sem,
    halo_recv_sem,
    known_sem,
    piece_recv_sem,
):
    gx, gy = lax.axis_index("gx"), lax.axis_index("gy")
    gx_lo, gx_hi = lax.rem(gx + gx_count - 1, gx_count), lax.rem(gx + 1, gx_count)
    gy_lo, gy_hi = lax.rem(gy + gy_count - 1, gy_count), lax.rem(gy + 1, gy_count)

    loads = [
        pltpu.make_async_copy(src, dst, local_sem.at[number])
        for number, (src, dst) in enumerate(
            ((head_in, head_a), (temp_in, temp_a), (cat_in, cat_a), (ice_in, ice_a))
        )
    ]
    params = [
        pltpu.make_async_copy(src, dst, local_sem.at[4 + number])
        for number, (src, dst) in enumerate(
            (
                (ks_in, ks_s),
                (alpha_in, alpha_s),
                (skew_in, skew_s),
                (steep_in, steep_s),
                (mid_in, mid_s),
                (order_in, order_s),
            )
        )
    ]
    for copy in params[:2] + loads + params[2:]:
        copy.start()

    px, py = lax.div(gy, 4), lax.rem(gy, 4)
    shifts = sorted(
        ((dx, dy) for dx in range(4) for dy in range(4) if (dx, dy) != (0, 0)),
        key=lambda d: -(min(d[0], 4 - d[0]) + min(d[1], 4 - d[1])),
    )
    peers = [lax.rem(px + dx, 4) * 4 + lax.rem(py + dy, 4) for dx, dy in shifts]

    has_x = (gx > 0, gx < gx_count - 1)
    has_y = (gy > 0, gy < gy_count - 1)
    x_at, y_at = (gx_lo, gx_hi), (gy_lo, gy_hi)
    both = [[jnp.logical_and(has_x[a], has_y[b]) for b in range(2)] for a in range(2)]
    is_hub = gy == HUB
    is_late = gy == HUB - 1
    far_from_hub = jnp.abs(gy - HUB) > 1

    barrier = pltpu.get_barrier_semaphore()

    def greet(device):
        pl.semaphore_signal(barrier, inc=1, device_id=device, device_id_type=MESH)

    def tell(number, device):
        pl.semaphore_signal(known_sem.at[number], inc=1, device_id=device, device_id_type=MESH)

    for a in range(2):

        @pl.when(both[a][0])
        def _():
            greet((x_at[a], gy_lo))

    @pl.when(has_y[0])
    def _():
        greet((gx, gy_lo))

    @pl.when(has_x[0])
    def _():
        greet((gx_lo, gy))

    @pl.when(far_from_hub)
    def _():
        greet((gx, HUB))

    def one(flag):
        return flag.astype(jnp.int32)

    x_sides = one(has_x[0]) + one(has_x[1])
    gathered = jnp.where(is_hub, gy_count - 3, 0)
    awaited = gathered + one(has_x[1]) + one(has_y[1]) * (1 + x_sides)

    @pl.when(awaited > 0)
    def _():
        pl.semaphore_wait(barrier, awaited)

    for a in range(2):

        @pl.when(both[a][1])
        def _():
            tell((CROSS, DIAGONAL)[a], (x_at[a], gy_hi))

    @pl.when(has_y[1])
    def _():
        tell(BELOW, (gx, gy_hi))

    @pl.when(has_x[1])
    def _():
        tell(BEFORE, (gx_hi, gy))

    @pl.when(is_hub)
    def _():
        for peer in peers:

            @pl.when(peer != HUB - 1)
            def _():
                tell(MOST, (gx, peer))

    row = lax.broadcasted_iota(jnp.int32, (SIDE, DEPTH), 0)
    lane = lax.broadcasted_iota(jnp.int32, (SIDE, DEPTH), 1)
    first, last = row == 0, row == SIDE - 1

    for copy in params[:2] + loads:
        copy.wait()

    def across(ref, y):
        return ref[pl.ds(y, SIDE, stride=SIDE), :]

    def tile(ref, x):
        return ref[pl.ds(x * SIDE, SIDE), :]

    head, temp, category, ice, ks, alpha, conduct = ({} for _ in range(7))

    def own(y):
        head[y], temp[y], category[y] = across(head_a, y), across(temp_a, y), across(cat_a, y)
        ice[y] = across(ice_a, y).astype(F32)
        ks[y], alpha[y] = lookup(category[y], ks_s), lookup(category[y], alpha_s)
        conduct[y] = conductivity(head[y], temp[y], ks[y], alpha[y], ice[y])

    for y in (0, 1, SIDE - 2, SIDE - 1):
        own(y)
    edge = {}
    for x in (0, 1, SIDE - 2, SIDE - 1):
        h, t, c = tile(head_a, x), tile(temp_a, x), tile(cat_a, x)
        i = tile(ice_a, x).astype(F32)
        k = conductivity(h, t, lookup(c, ks_s), lookup(c, alpha_s), i)
        edge[x] = (h, t, c.astype(F32), i, k)

    for side, (near, far) in enumerate(((0, 1), (SIDE - 1, SIDE - 2))):
        parts = (
            head[near],
            temp[near],
            category[near].astype(F32),
            ice[near],
            head[far],
            temp[far],
            conduct[far],
        )
        for number, part in enumerate(parts):
            y_send[side, pl.ds(number * SIDE, SIDE), :] = part
        parts = (*edge[near][:4], edge[far][0], edge[far][1], edge[far][4])
        for number, part in enumerate(parts):
            x_send[side, pl.ds(number * SIDE, SIDE), :] = part
    for number, (x, y) in enumerate(((0, 0), (0, 7), (7, 0), (7, 7))):
        for field, part in enumerate((head[y], temp[y], conduct[y], conduct[y])):
            c_send[number // 2, number % 2, pl.ds(field, 1), :] = part[x : x + 1, :]

    def remote(src, dst, mine, theirs, device):
        return pltpu.make_async_remote_copy(
            src_ref=src,
            dst_ref=dst,
            send_sem=local_sem.at[(0, 1, 2, 3, 4, 5, 10, 11)[mine]],
            recv_sem=halo_recv_sem.at[theirs],
            device_id=device,
            device_id_type=MESH,
        )

    def y_copy(b):
        return remote(y_send.at[b], y_recv.at[1 - b], b, 1 - b, (gx, y_at[b]))

    def x_copy(a):
        return remote(x_send.at[a], x_recv.at[1 - a], 2 + a, 3 - a, (x_at[a], gy))

    def c_copy(a, b):
        slot = 4 + 2 * a + b
        return remote(
            c_send.at[a, b], c_recv.at[1 - a, 1 - b], slot, 11 - slot, (x_at[a], y_at[b])
        )

    def send(present, copy, *known):
        @pl.when(present)
        def _():
            for number in known:
                pl.semaphore_wait(known_sem.at[number], 1)
            copy.start()

    for a in range(2):
        send(both[a][1], c_copy(a, 1))
    send(has_y[1], y_copy(1))
    send(has_x[1], x_copy(1))
    send(has_x[0], x_copy(0), BEFORE)
    send(both[1][0], c_copy(1, 0), CROSS)
    send(has_y[0], y_copy(0), BELOW)

    @pl.when(is_hub)
    def _():
        for peer in peers:
            tell(ALL, (gx, peer))

    send(both[0][0], c_copy(0, 0), DIAGONAL)

    for copy in params[2:]:
        copy.wait()

    x_open = (jnp.logical_or(row > 0, has_x[0]), jnp.logical_or(row < SIDE - 1, has_x[1]))
    y_open = (jnp.logical_or(row > 0, has_y[0]), jnp.logical_or(row < SIDE - 1, has_y[1]))

    for y in range(2, SIDE - 2):
        own(y)

    def arrived(a, b):
        slot = 4 + 2 * a + b
        return remote(c_send.at[a, b], c_recv.at[a, b], slot, slot, (gx, gy_lo))

    x_waits = [
        (has_x[a], remote(x_send.at[a], x_recv.at[a], 2 + a, 2 + a, (gx, gy_lo)))
        for a in range(2)
    ]
    y_waits = [(both[a][b], arrived(a, b)) for a in range(2) for b in range(2)]
    y_waits += [
        (has_y[b], remote(y_send.at[b], y_recv.at[b], b, b, (gx, gy_lo))) for b in range(2)
    ]

    def receive(waits):
        for present, copy in waits:

            @pl.when(present)
            def _():
                copy.wait_recv()

    def along_rows(value, before, after):
        return (
            jnp.where(first, before, pltpu.roll(value, 1, 0)),
            jnp.where(last, after, pltpu.roll(value, SIDE - 1, 0)),
        )

    def change_rows(head_, conduct_, temp_, ends, opened):
        (h_lo, t_lo, k_lo), (h_hi, t_hi, k_hi) = ends
        heads = along_rows(head_, h_lo, h_hi)
        temps = along_rows(temp_, t_lo, t_hi)
        conducts = along_rows(conduct_, k_lo, k_hi)
        total = sum(
            jnp.where(opened[s], (conduct_ + conducts[s]) * (heads[s] - head_), 0.0)
            for s in range(2)
        )
        return total, temps[0] + temps[1]

    def y_part(side, number):
        return y_recv[side, pl.ds(number * SIDE, SIDE), :]

    def x_part(side, number):
        return x_recv[side, pl.ds(number * SIDE, SIDE), :]

    def warm_if(present, value):
        return jnp.where(present, value, 0.0)

    def corner(xs, ys):
        return (
            c_recv[xs, ys, pl.ds(0, 1), :],
            warm_if(jnp.logical_and(has_x[xs], has_y[ys]), c_recv[xs, ys, pl.ds(1, 1), :]),
            c_recv[xs, ys, pl.ds(2, 1), :],
        )

    def read_ghost(part_of, side, present):
        h, t, c, i = (part_of(side, number) for number in range(4))
        k_s, a = lookup(c, ks_s), lookup(c, alpha_s)
        far = tuple(part_of(side, number) for number in range(4, 7))
        return h, warm_if(present, t), conductivity(h, t, k_s, a, i), k_s, a, i, far

    def step(h, t, change, warm):
        return h + 0.5 * change, t + DIFFUSE * (warm - 6.0 * t)

    def face(k_a, h_a, k_b, h_b):
        return (k_a + k_b) * (h_b - h_a)

    def ghost_base(cell, inner):
        h, t, k, far = cell[0], cell[1], cell[2], cell[6]
        change, warm = vertical(h, t, k, lane)
        change = change + face(k, h, far[2], far[0]) + face(k, h, inner[2], inner[0])
        return change, warm + far[1] + inner[1]

    def ghost_step(cell, base, ends, opened, present):
        h, t, k, k_s, a, i, _ = cell
        rows, rows_warm = change_rows(h, k, t, ends, opened)
        h, t = step(h, t, base[0] + rows, base[1] + rows_warm)
        return h, warm_if(present, t), conductivity(h, t, k_s, a, i)

    def keep(slot, cells):
        for side in range(2):
            for field in range(3):
                ghost[slot + side, field] = cells[side][field]

    def base_of(y, h, t, k, slot):
        ends = tuple(
            tuple(ghost[slot + side, field, pl.ds(y, 1), :] for field in range(3))
            for side in range(2)
        )
        change, warm = vertical(h[y], t[y], k[y], lane)
        rows, rows_warm = change_rows(h[y], k[y], t[y], ends, x_open)
        return change + rows, warm + rows_warm

    def plane_step(y, h, t, k, base, faces):
        for edge_ in (y, y + 1):
            if edge_ not in faces:
                value = face(k[edge_ - 1], h[edge_ - 1], k[edge_], h[edge_])
                if edge_ in (0, SIDE):
                    value = jnp.where(has_y[edge_ // SIDE], value, 0.0)
                faces[edge_] = value
        return step(
            h[y],
            t[y],
            base[0] + faces[y + 1] - faces[y],
            base[1] + t[y - 1] + t[y + 1],
        )

    planes_all = gy_count * SIDE

    def view_planes(view, planes, theta):
        clear = depth = None
        sums = [None] * 3
        for y in planes:
            shift = skew_s[view] * ((gy * SIDE + y).astype(F32) - 0.5 * planes_all)
            wrapped = shift - DEPTH * jnp.floor(shift * (1.0 / DEPTH))
            base = jnp.floor(wrapped)
            part = wrapped - base
            turn = lax.rem(2 * DEPTH - base.astype(jnp.int32), DEPTH)
            lower = pltpu.roll(theta[y], turn, 1)
            upper = pltpu.roll(theta[y], lax.rem(turn + DEPTH - 1, DEPTH), 1)
            sample = (1.0 - part) * lower + part * upper
            optical = sample * (8.0 / planes_all)
            passed = jnp.exp(-optical)
            after = passed if clear is None else clear * passed
            weight = (1.0 if clear is None else clear) - after
            clear = after
            depth = optical if depth is None else depth + optical
            for color in range(3):
                term = weight * jnp.tanh((0.5 * steep_s[color]) * (sample - mid_s[color]))
                sums[color] = term if sums[color] is None else sums[color] + term
        return clear, sums, depth

    theta = {}

    def finish(y, h, t):
        head_v[pl.ds(y, SIDE, stride=SIDE), :] = h
        temp_v[pl.ds(y, SIDE, stride=SIDE), :] = t
        theta[y] = 0.05 + 0.4 * jnp.exp(0.8 * jnp.minimum(h, 0.0))

    receive(x_waits)
    x_ghost = [read_ghost(x_part, side, has_x[side]) for side in range(2)]
    keep(0, x_ghost)
    bases = [base_of(y, head, temp, conduct, 0) for y in range(SIDE)]
    faces, head_1, temp_1, conduct_1 = {}, {}, {}, {}

    def first_step(y):
        head_1[y], temp_1[y] = plane_step(y, head, temp, conduct, bases[y], faces)
        conduct_1[y] = conductivity(head_1[y], temp_1[y], ks[y], alpha[y], ice[y])

    for y in range(1, SIDE - 1):
        first_step(y)
    x_bases = [
        ghost_base(x_ghost[side], (edge[x][0], edge[x][1], edge[x][4]))
        for side, x in ((0, 0), (1, SIDE - 1))
    ]
    nothing = jnp.zeros((1, DEPTH), F32)
    keep(
        2,
        [
            ghost_step(x_ghost[side], x_bases[side], ((nothing,) * 3,) * 2, y_open, has_x[side])
            for side in range(2)
        ],
    )
    bases_1 = {y: base_of(y, head_1, temp_1, conduct_1, 2) for y in range(1, SIDE - 1)}
    faces_1 = {}
    middle = range(2, SIDE - 2)
    for y in middle:
        finish(y, *plane_step(y, head_1, temp_1, conduct_1, bases_1[y], faces_1))
    middles = [view_planes(view, middle, theta) for view in range(VIEWS)]

    receive(y_waits)
    y_ghost = [read_ghost(y_part, side, has_y[side]) for side in range(2)]
    for side, y in ((0, -1), (1, SIDE)):
        head[y], temp[y], conduct[y] = y_ghost[side][:3]
    for y in (0, SIDE - 1):
        first_step(y)
    for side, y, out in ((0, 0, -1), (1, SIDE - 1, SIDE)):
        head_1[out], temp_1[out], conduct_1[out] = ghost_step(
            y_ghost[side],
            ghost_base(y_ghost[side], (head[y], temp[y], conduct[y])),
            (corner(0, side), corner(1, side)),
            x_open,
            has_y[side],
        )
    keep(
        4,
        [
            ghost_step(
                x_ghost[side],
                x_bases[side],
                (corner(side, 0), corner(side, 1)),
                y_open,
                has_x[side],
            )
            for side in range(2)
        ],
    )
    for y in (0, SIDE - 1):
        bases_1[y] = base_of(y, head_1, temp_1, conduct_1, 4)
    for y in (0, 1, SIDE - 2, SIDE - 1):
        finish(y, *plane_step(y, head_1, temp_1, conduct_1, bases_1[y], faces_1))

    layers = []
    for view in range(VIEWS):
        clear_a, sums_a, depth_a = view_planes(view, (0, 1), theta)
        clear_b, sums_b, depth_b = middles[view]
        clear_c, sums_c, depth_c = view_planes(view, (SIDE - 2, SIDE - 1), theta)
        opaque = 1.0 - clear_a * (clear_b * clear_c)
        for color in range(3):
            total = sums_a[color] + clear_a * (sums_b[color] + clear_b * sums_c[color])
            layers.append(0.5 * (opaque + total))
        layers.append(depth_a + depth_b + depth_c)
    piece_send[...] = jnp.transpose(jnp.concatenate(layers, 0))

    among_late = jnp.where(gy < LATE, 1, 0)

    def exchange(src, dst, device):
        return pltpu.make_async_remote_copy(
            src_ref=src,
            dst_ref=dst,
            send_sem=local_sem.at[6],
            recv_sem=piece_recv_sem.at[among_late],
            device_id=device,
            device_id_type=MESH,
        )

    plain = jnp.logical_not(jnp.logical_or(is_hub, is_late))

    def give(peer):
        exchange(
            piece_send.at[pl.ds(pl.multiple_of(peer * SIDE, SIDE), SIDE)],
            piece_recv.at[gy],
            (gx, peer),
        ).start()

    @pl.when(plain)
    def _():
        pl.semaphore_wait(known_sem.at[MOST], 1)

    @pl.when(is_late)
    def _():
        pl.semaphore_wait(known_sem.at[ALL], 1)

    for peer in peers:

        @pl.when(peer != HUB - 1)
        def _():
            give(peer)

    @pl.when(plain)
    def _():
        pl.semaphore_wait(known_sem.at[ALL], 1)

    @pl.when(jnp.logical_not(is_late))
    def _():
        give(HUB - 1)

    piece_recv[gy] = piece_send[pl.ds(pl.multiple_of(gy * SIDE, SIDE), SIDE), :]

    view_of = lax.div(lane, 4 * SIDE)
    kind_of = lax.rem(lax.div(lane, SIDE), 4)
    ranks = []
    for group in range(GROUPS):
        rank = jnp.full((SIDE, DEPTH), order_s[0, group], jnp.int32)
        for view in range(1, VIEWS):
            rank = jnp.where(view_of == view, order_s[view, group], rank)
        ranks.append(rank)
    is_depth = kind_of == 3

    def arrive(number, tiles):
        slots = piece_recv.at[pl.ds(0, tiles)]
        pltpu.make_async_remote_copy(
            src_ref=slots,
            dst_ref=slots,
            send_sem=local_sem.at[6],
            recv_sem=piece_recv_sem.at[number],
            device_id=(gx, gy_lo),
            device_id_type=MESH,
        ).wait_recv()

    depths, fronts = {}, {}

    def place(group):
        value = jnp.where(is_depth, piece_recv[group], 0.0)
        value = value + pltpu.roll(value, DEPTH - SIDE, 1)
        depths[group] = value + pltpu.roll(value, DEPTH - 2 * SIDE, 1)
        total = jnp.zeros((SIDE, DEPTH), F32)
        for other in fronts:
            before = ranks[other] < ranks[group]
            total = total + jnp.where(before, depths[other], 0.0)
            fronts[other] = fronts[other] + jnp.where(before, 0.0, depths[group])
        fronts[group] = total

    for number, groups, tiles in ((0, range(LATE, GROUPS), GROUPS - LATE), (1, range(LATE), LATE)):
        own_late = among_late == number

        @pl.when(own_late)
        def _():
            arrive(number, tiles - 1)

        @pl.when(jnp.logical_not(own_late))
        def _():
            arrive(number, tiles)

        for group in groups:
            place(group)
    color = sum(jnp.exp(-fronts[group]) * piece_recv[group] for group in range(GROUPS))
    opaque = 1.0 - jnp.exp(-sum(depths.values()))
    image_v[...] = jnp.transpose(jnp.where(is_depth, opaque, color))
    for present, copy in x_waits + y_waits:

        @pl.when(present)
        def _():
            copy.wait_send()

    sent = piece_recv.at[pl.ds(0, GROUPS - 1)]
    pltpu.make_async_remote_copy(
        src_ref=sent,
        dst_ref=sent,
        send_sem=local_sem.at[6],
        recv_sem=piece_recv_sem.at[0],
        device_id=(gx, gy_lo),
        device_id_type=MESH,
    ).wait_send()


def put_out(head_v, temp_v, image_v, head_out, temp_out, image_out, sem):
    copies = [
        pltpu.make_async_copy(src, dst, sem.at[number])
        for number, (src, dst) in enumerate(
            ((image_v, image_out), (head_v, head_out), (temp_v, temp_out))
        )
    ]
    for copy in copies:
        copy.start()
    for copy in copies:
        copy.wait()


def shards(head, temp, category, ice, *params):
    gx_count, gy_count = lax.axis_size("gx"), lax.axis_size("gy")
    rows = SIDE * SIDE
    flat = [a.reshape(rows, DEPTH) for a in (head, temp, category, ice)]
    vmem = pltpu.VMEM
    dma = pltpu.SemaphoreType.DMA
    shapes = ((rows, DEPTH), (rows, DEPTH), (DEPTH, SIDE))
    results = pl.pallas_call(
        functools.partial(kernel, gx_count, gy_count),
        out_shape=tuple(pltpu.VMEM(shape, F32) for shape in shapes),
        in_specs=[pl.BlockSpec(memory_space=pl.ANY)] * 10,
        out_specs=[pl.BlockSpec(memory_space=pltpu.VMEM)] * 3,
        scratch_shapes=[
            vmem((rows, DEPTH), F32),
            vmem((rows, DEPTH), F32),
            vmem((rows, DEPTH), jnp.int32),
            vmem((rows, DEPTH), jnp.int32),
            pltpu.SMEM((SOILS,), F32),
            pltpu.SMEM((SOILS,), F32),
            pltpu.SMEM((VIEWS,), F32),
            pltpu.SMEM((3,), F32),
            pltpu.SMEM((3,), F32),
            pltpu.SMEM((VIEWS, GROUPS), jnp.int32),
            vmem((2, 7 * SIDE, DEPTH), F32),
            vmem((2, 7 * SIDE, DEPTH), F32),
            vmem((2, 7 * SIDE, DEPTH), F32),
            vmem((2, 7 * SIDE, DEPTH), F32),
            vmem((2, 2, 4, DEPTH), F32),
            vmem((2, 2, 4, DEPTH), F32),
            vmem((6, 3, SIDE, DEPTH), F32),
            vmem((DEPTH, DEPTH), F32),
            vmem((GROUPS, SIDE, DEPTH), F32),
            dma((12,)),
            dma((8,)),
            pltpu.SemaphoreType.REGULAR((6,)),
            dma((2,)),
        ],
        compiler_params=pltpu.CompilerParams(collective_id=0, has_side_effects=True),
        name="step_and_view",
    )(*flat, *params)
    head, temp, image = pl.pallas_call(
        put_out,
        out_shape=tuple(jax.ShapeDtypeStruct(shape, F32) for shape in shapes),
        in_specs=[pl.BlockSpec(memory_space=pltpu.VMEM)] * 3,
        out_specs=[pl.BlockSpec(memory_space=pl.ANY)] * 3,
        scratch_shapes=[dma((3,))],
        name="put_out",
    )(*(pltpu.with_memory_space_constraint(r, pltpu.VMEM) for r in results))
    shape = (SIDE, SIDE, DEPTH)
    return head.reshape(shape), temp.reshape(shape), image.reshape(VIEWS, 4, SIDE, SIDE)


def solution(mesh):
    block = P("gx", "gy", None)
    return jax.shard_map(
        shards,
        mesh=mesh,
        in_specs=(block,) * 4 + (P(),) * 6,
        out_specs=(block, block, P(None, None, "gx", "gy")),
        check_vma=False,
    )
```

```python
import functools

import jax
import jax.numpy as jnp
from jax import lax
from jax.experimental import pallas as pl
from jax.experimental.pallas import tpu as pltpu
from jax.sharding import PartitionSpec as P

MESH = pl.DeviceIdType.MESH
SOILS = 12
VIEWS = 4
SIDE = 8
DEPTH = 128
GROUPS = 16
DIFFUSE = 0.12
HUB = 1
LATE = 2
BEFORE, CROSS, BELOW, DIAGONAL, MOST, ALL = range(6)
F32 = jnp.float32


def lookup(category, table):
    total = jnp.full(category.shape, table[0], F32)
    for number in range(1, SOILS):
        total = jnp.where(category == number, table[number], total)
    return total


def conductivity(head, temp, ks, alpha, ice):
    return ks * jnp.exp(alpha * jnp.minimum(head, 0.0) + 2.0 * ice * (jnp.tanh(temp) - 1.0))


def face(k_a, h_a, k_b, h_b):
    return (k_a + k_b) * (h_b - h_a)


def vertical(head, temp, conduct, lane):
    inner_lo, inner_hi = lane > 0, lane < DEPTH - 1
    above, conduct_above = (pltpu.roll(a, DEPTH - 1, 1) for a in (head, conduct))
    below, conduct_below = (pltpu.roll(a, 1, 1) for a in (head, conduct))
    change = jnp.where(inner_hi, (conduct + conduct_above) * (above - head + 1.0), 0.0) - jnp.where(
        inner_lo, (conduct + conduct_below) * (head - below + 1.0), 0.0
    )
    warm = jnp.where(inner_hi, pltpu.roll(temp, DEPTH - 1, 1), 0.0) + jnp.where(
        inner_lo, pltpu.roll(temp, 1, 1), 0.0
    )
    return change, warm


def kernel(
    gx_count,
    gy_count,
    head_in,
    temp_in,
    cat_in,
    ice_in,
    ks_in,
    alpha_in,
    skew_in,
    steep_in,
    mid_in,
    order_in,
    head_v,
    temp_v,
    image_v,
    head_a,
    temp_a,
    cat_a,
    ice_a,
    ks_s,
    alpha_s,
    skew_s,
    steep_s,
    mid_s,
    order_s,
    y_send,
    y_recv,
    x_send,
    x_recv,
    c_send,
    c_recv,
    ghost,
    piece_send,
    piece_recv,
    local_sem,
    halo_recv_sem,
    known_sem,
    piece_recv_sem,
):
    gx, gy = lax.axis_index("gx"), lax.axis_index("gy")
    gx_lo, gx_hi = lax.rem(gx + gx_count - 1, gx_count), lax.rem(gx + 1, gx_count)
    gy_lo, gy_hi = lax.rem(gy + gy_count - 1, gy_count), lax.rem(gy + 1, gy_count)

    loads = [
        pltpu.make_async_copy(src, dst, local_sem.at[number])
        for number, (src, dst) in enumerate(
            ((head_in, head_a), (temp_in, temp_a), (cat_in, cat_a), (ice_in, ice_a))
        )
    ]
    params = [
        pltpu.make_async_copy(src, dst, local_sem.at[4 + number])
        for number, (src, dst) in enumerate(
            (
                (ks_in, ks_s),
                (alpha_in, alpha_s),
                (skew_in, skew_s),
                (steep_in, steep_s),
                (mid_in, mid_s),
                (order_in, order_s),
            )
        )
    ]
    for copy in params[:2] + loads + params[2:]:
        copy.start()

    px, py = lax.div(gy, 4), lax.rem(gy, 4)
    shifts = sorted(
        ((dx, dy) for dx in range(4) for dy in range(4) if (dx, dy) != (0, 0)),
        key=lambda d: -(min(d[0], 4 - d[0]) + min(d[1], 4 - d[1])),
    )
    peers = [lax.rem(px + dx, 4) * 4 + lax.rem(py + dy, 4) for dx, dy in shifts]

    has_x = (gx > 0, gx < gx_count - 1)
    has_y = (gy > 0, gy < gy_count - 1)
    x_at, y_at = (gx_lo, gx_hi), (gy_lo, gy_hi)
    both = [[jnp.logical_and(has_x[a], has_y[b]) for b in range(2)] for a in range(2)]
    is_hub = gy == HUB
    is_late = gy == HUB - 1
    far_from_hub = jnp.abs(gy - HUB) > 1

    barrier = pltpu.get_barrier_semaphore()

    def greet(device):
        pl.semaphore_signal(barrier, inc=1, device_id=device, device_id_type=MESH)

    def tell(number, device):
        pl.semaphore_signal(known_sem.at[number], inc=1, device_id=device, device_id_type=MESH)

    for a in range(2):

        @pl.when(both[a][0])
        def _():
            greet((x_at[a], gy_lo))

    @pl.when(has_y[0])
    def _():
        greet((gx, gy_lo))

    @pl.when(has_x[0])
    def _():
        greet((gx_lo, gy))

    @pl.when(far_from_hub)
    def _():
        greet((gx, HUB))

    def one(flag):
        return flag.astype(jnp.int32)

    x_sides = one(has_x[0]) + one(has_x[1])
    gathered = jnp.where(is_hub, gy_count - 3, 0)
    awaited = gathered + one(has_x[1]) + one(has_y[1]) * (1 + x_sides)

    @pl.when(awaited > 0)
    def _():
        pl.semaphore_wait(barrier, awaited)

    for a in range(2):

        @pl.when(both[a][1])
        def _():
            tell((CROSS, DIAGONAL)[a], (x_at[a], gy_hi))

    @pl.when(has_y[1])
    def _():
        tell(BELOW, (gx, gy_hi))

    @pl.when(has_x[1])
    def _():
        tell(BEFORE, (gx_hi, gy))

    @pl.when(is_hub)
    def _():
        for peer in peers:

            @pl.when(peer != HUB - 1)
            def _():
                tell(MOST, (gx, peer))

    row = lax.broadcasted_iota(jnp.int32, (SIDE, DEPTH), 0)
    lane = lax.broadcasted_iota(jnp.int32, (SIDE, DEPTH), 1)
    first, last = row == 0, row == SIDE - 1

    for copy in params[:2] + loads:
        copy.wait()

    def across(ref, y):
        return ref[pl.ds(y, SIDE, stride=SIDE), :]

    def tile(ref, x):
        return ref[pl.ds(x * SIDE, SIDE), :]

    head, temp, category, ice, ks, alpha, conduct = ({} for _ in range(7))

    def own(y):
        head[y], temp[y], category[y] = across(head_a, y), across(temp_a, y), across(cat_a, y)
        ice[y] = across(ice_a, y).astype(F32)
        ks[y], alpha[y] = lookup(category[y], ks_s), lookup(category[y], alpha_s)
        conduct[y] = conductivity(head[y], temp[y], ks[y], alpha[y], ice[y])

    def remote(src, dst, mine, theirs, device):
        return pltpu.make_async_remote_copy(
            src_ref=src,
            dst_ref=dst,
            send_sem=local_sem.at[(0, 1, 2, 3, 4, 5, 10, 11)[mine]],
            recv_sem=halo_recv_sem.at[theirs],
            device_id=device,
            device_id_type=MESH,
        )

    def y_copy(b):
        return remote(y_send.at[b], y_recv.at[1 - b], b, 1 - b, (gx, y_at[b]))

    def x_copy(a):
        return remote(x_send.at[a], x_recv.at[1 - a], 2 + a, 3 - a, (x_at[a], gy))

    def c_copy(a, b):
        slot = 4 + 2 * a + b
        return remote(
            c_send.at[a, b], c_recv.at[1 - a, 1 - b], slot, 11 - slot, (x_at[a], y_at[b])
        )

    def send(present, copy, *known):
        @pl.when(present)
        def _():
            for number in known:
                pl.semaphore_wait(known_sem.at[number], 1)
            copy.start()

    def stage_y(side):
        near, far = ((0, 1), (SIDE - 1, SIDE - 2))[side]
        own(near)
        own(far)
        parts = (
            head[near],
            temp[near],
            category[near].astype(F32),
            ice[near],
            face(conduct[near], head[near], conduct[far], head[far]),
            temp[far],
        )
        for number, part in enumerate(parts):
            y_send[side, pl.ds(number * SIDE, SIDE), :] = part
        for a, x in enumerate((0, SIDE - 1)):
            for field, part in enumerate((head[near], temp[near], conduct[near], conduct[near])):
                c_send[a, side, pl.ds(field, 1), :] = part[x : x + 1, :]

    stage_y(1)
    for a in range(2):
        send(both[a][1], c_copy(a, 1))
    send(has_y[1], y_copy(1))

    edge = {}
    for x in (0, 1, SIDE - 2, SIDE - 1):
        h, t, c = tile(head_a, x), tile(temp_a, x), tile(cat_a, x)
        i = tile(ice_a, x).astype(F32)
        k = conductivity(h, t, lookup(c, ks_s), lookup(c, alpha_s), i)
        edge[x] = (h, t, c.astype(F32), i, k)
    for side, (near, far) in enumerate(((0, 1), (SIDE - 1, SIDE - 2))):
        inner, outer = edge[far], edge[near]
        parts = (*outer[:4], face(outer[4], outer[0], inner[4], inner[0]), inner[1])
        for number, part in enumerate(parts):
            x_send[side, pl.ds(number * SIDE, SIDE), :] = part
    send(has_x[1], x_copy(1))
    stage_y(0)
    send(has_x[0], x_copy(0), BEFORE)
    send(both[1][0], c_copy(1, 0), CROSS)
    send(has_y[0], y_copy(0), BELOW)

    @pl.when(is_hub)
    def _():
        for peer in peers:
            tell(ALL, (gx, peer))

    send(both[0][0], c_copy(0, 0), DIAGONAL)

    for copy in params[2:]:
        copy.wait()

    x_open = (jnp.logical_or(row > 0, has_x[0]), jnp.logical_or(row < SIDE - 1, has_x[1]))
    y_open = (jnp.logical_or(row > 0, has_y[0]), jnp.logical_or(row < SIDE - 1, has_y[1]))

    for y in range(2, SIDE - 2):
        own(y)

    def arrived(a, b):
        slot = 4 + 2 * a + b
        return remote(c_send.at[a, b], c_recv.at[a, b], slot, slot, (gx, gy_lo))

    x_waits = [
        (has_x[a], remote(x_send.at[a], x_recv.at[a], 2 + a, 2 + a, (gx, gy_lo)))
        for a in range(2)
    ]
    y_waits = [(both[a][b], arrived(a, b)) for a in range(2) for b in range(2)]
    y_waits += [
        (has_y[b], remote(y_send.at[b], y_recv.at[b], b, b, (gx, gy_lo))) for b in range(2)
    ]

    def receive(waits):
        for present, copy in waits:

            @pl.when(present)
            def _():
                copy.wait_recv()

    def along_rows(value, before, after):
        return (
            jnp.where(first, before, pltpu.roll(value, 1, 0)),
            jnp.where(last, after, pltpu.roll(value, SIDE - 1, 0)),
        )

    def change_rows(head_, conduct_, temp_, ends, opened):
        (h_lo, t_lo, k_lo), (h_hi, t_hi, k_hi) = ends
        heads = along_rows(head_, h_lo, h_hi)
        temps = along_rows(temp_, t_lo, t_hi)
        conducts = along_rows(conduct_, k_lo, k_hi)
        total = sum(
            jnp.where(opened[s], (conduct_ + conducts[s]) * (heads[s] - head_), 0.0)
            for s in range(2)
        )
        return total, temps[0] + temps[1]

    def y_part(side, number):
        return y_recv[side, pl.ds(number * SIDE, SIDE), :]

    def x_part(side, number):
        return x_recv[side, pl.ds(number * SIDE, SIDE), :]

    def warm_if(present, value):
        return jnp.where(present, value, 0.0)

    def corner(xs, ys):
        return (
            c_recv[xs, ys, pl.ds(0, 1), :],
            warm_if(jnp.logical_and(has_x[xs], has_y[ys]), c_recv[xs, ys, pl.ds(1, 1), :]),
            c_recv[xs, ys, pl.ds(2, 1), :],
        )

    def read_ghost(part_of, side, present):
        h, t, c, i = (part_of(side, number) for number in range(4))
        k_s, a = lookup(c, ks_s), lookup(c, alpha_s)
        far = tuple(part_of(side, number) for number in range(4, 6))
        return h, warm_if(present, t), conductivity(h, t, k_s, a, i), k_s, a, i, far

    def step(h, t, change, warm):
        return h + 0.5 * change, t + DIFFUSE * (warm - 6.0 * t)

    def ghost_base(cell, inner):
        h, t, k, far = cell[0], cell[1], cell[2], cell[6]
        change, warm = vertical(h, t, k, lane)
        change = change + far[0] + face(k, h, inner[2], inner[0])
        return change, warm + far[1] + inner[1]

    def ghost_step(cell, base, ends, opened, present):
        h, t, k, k_s, a, i, _ = cell
        rows, rows_warm = change_rows(h, k, t, ends, opened)
        h, t = step(h, t, base[0] + rows, base[1] + rows_warm)
        return h, warm_if(present, t), conductivity(h, t, k_s, a, i)

    def keep(slot, cells):
        for side in range(2):
            for field in range(3):
                ghost[slot + side, field] = cells[side][field]

    def base_of(y, h, t, k, slot):
        ends = tuple(
            tuple(ghost[slot + side, field, pl.ds(y, 1), :] for field in range(3))
            for side in range(2)
        )
        change, warm = vertical(h[y], t[y], k[y], lane)
        rows, rows_warm = change_rows(h[y], k[y], t[y], ends, x_open)
        return change + rows, warm + rows_warm

    def plane_step(y, h, t, k, base, faces):
        for edge_ in (y, y + 1):
            if edge_ not in faces:
                value = face(k[edge_ - 1], h[edge_ - 1], k[edge_], h[edge_])
                if edge_ in (0, SIDE):
                    value = jnp.where(has_y[edge_ // SIDE], value, 0.0)
                faces[edge_] = value
        return step(
            h[y],
            t[y],
            base[0] + faces[y + 1] - faces[y],
            base[1] + t[y - 1] + t[y + 1],
        )

    planes_all = gy_count * SIDE

    def view_planes(view, planes, theta):
        clear = depth = None
        sums = [None] * 3
        for y in planes:
            shift = skew_s[view] * ((gy * SIDE + y).astype(F32) - 0.5 * planes_all)
            wrapped = shift - DEPTH * jnp.floor(shift * (1.0 / DEPTH))
            base = jnp.floor(wrapped)
            part = wrapped - base
            turn = lax.rem(2 * DEPTH - base.astype(jnp.int32), DEPTH)
            lower = pltpu.roll(theta[y], turn, 1)
            upper = pltpu.roll(theta[y], lax.rem(turn + DEPTH - 1, DEPTH), 1)
            sample = (1.0 - part) * lower + part * upper
            optical = sample * (8.0 / planes_all)
            passed = jnp.exp(-optical)
            after = passed if clear is None else clear * passed
            weight = (1.0 if clear is None else clear) - after
            clear = after
            depth = optical if depth is None else depth + optical
            for color in range(3):
                term = weight * jnp.tanh((0.5 * steep_s[color]) * (sample - mid_s[color]))
                sums[color] = term if sums[color] is None else sums[color] + term
        return clear, sums, depth

    theta = {}

    def finish(y, h, t):
        head_v[pl.ds(y, SIDE, stride=SIDE), :] = h
        temp_v[pl.ds(y, SIDE, stride=SIDE), :] = t
        theta[y] = 0.05 + 0.4 * jnp.exp(0.8 * jnp.minimum(h, 0.0))

    receive(x_waits)
    x_ghost = [read_ghost(x_part, side, has_x[side]) for side in range(2)]
    keep(0, x_ghost)
    bases = [base_of(y, head, temp, conduct, 0) for y in range(SIDE)]
    faces, head_1, temp_1, conduct_1 = {}, {}, {}, {}

    def first_step(y):
        head_1[y], temp_1[y] = plane_step(y, head, temp, conduct, bases[y], faces)
        conduct_1[y] = conductivity(head_1[y], temp_1[y], ks[y], alpha[y], ice[y])

    for y in range(1, SIDE - 1):
        first_step(y)
    x_bases = [
        ghost_base(x_ghost[side], (edge[x][0], edge[x][1], edge[x][4]))
        for side, x in ((0, 0), (1, SIDE - 1))
    ]
    nothing = jnp.zeros((1, DEPTH), F32)
    keep(
        2,
        [
            ghost_step(x_ghost[side], x_bases[side], ((nothing,) * 3,) * 2, y_open, has_x[side])
            for side in range(2)
        ],
    )
    bases_1 = {y: base_of(y, head_1, temp_1, conduct_1, 2) for y in range(1, SIDE - 1)}
    faces_1 = {}
    middle = range(2, SIDE - 2)
    for y in middle:
        finish(y, *plane_step(y, head_1, temp_1, conduct_1, bases_1[y], faces_1))
    middles = [view_planes(view, middle, theta) for view in range(VIEWS)]

    receive(y_waits)
    y_ghost = [read_ghost(y_part, side, has_y[side]) for side in range(2)]
    for side, y in ((0, -1), (1, SIDE)):
        head[y], temp[y], conduct[y] = y_ghost[side][:3]
    for y in (0, SIDE - 1):
        first_step(y)
    for side, y, out in ((0, 0, -1), (1, SIDE - 1, SIDE)):
        head_1[out], temp_1[out], conduct_1[out] = ghost_step(
            y_ghost[side],
            ghost_base(y_ghost[side], (head[y], temp[y], conduct[y])),
            (corner(0, side), corner(1, side)),
            x_open,
            has_y[side],
        )
    keep(
        4,
        [
            ghost_step(
                x_ghost[side],
                x_bases[side],
                (corner(side, 0), corner(side, 1)),
                y_open,
                has_x[side],
            )
            for side in range(2)
        ],
    )
    for y in (0, SIDE - 1):
        bases_1[y] = base_of(y, head_1, temp_1, conduct_1, 4)
    for y in (0, 1, SIDE - 2, SIDE - 1):
        finish(y, *plane_step(y, head_1, temp_1, conduct_1, bases_1[y], faces_1))

    layers = []
    for view in range(VIEWS):
        clear_a, sums_a, depth_a = view_planes(view, (0, 1), theta)
        clear_b, sums_b, depth_b = middles[view]
        clear_c, sums_c, depth_c = view_planes(view, (SIDE - 2, SIDE - 1), theta)
        opaque = 1.0 - clear_a * (clear_b * clear_c)
        for color in range(3):
            total = sums_a[color] + clear_a * (sums_b[color] + clear_b * sums_c[color])
            layers.append(0.5 * (opaque + total))
        layers.append(depth_a + depth_b + depth_c)
    piece_send[...] = jnp.transpose(jnp.concatenate(layers, 0))

    among_late = jnp.where(gy < LATE, 1, 0)

    def exchange(src, dst, device):
        return pltpu.make_async_remote_copy(
            src_ref=src,
            dst_ref=dst,
            send_sem=local_sem.at[6],
            recv_sem=piece_recv_sem.at[among_late],
            device_id=device,
            device_id_type=MESH,
        )

    plain = jnp.logical_not(jnp.logical_or(is_hub, is_late))

    def give(peer):
        exchange(
            piece_send.at[pl.ds(pl.multiple_of(peer * SIDE, SIDE), SIDE)],
            piece_recv.at[gy],
            (gx, peer),
        ).start()

    @pl.when(plain)
    def _():
        pl.semaphore_wait(known_sem.at[MOST], 1)

    @pl.when(is_late)
    def _():
        pl.semaphore_wait(known_sem.at[ALL], 1)

    for peer in peers:

        @pl.when(peer != HUB - 1)
        def _():
            give(peer)

    @pl.when(plain)
    def _():
        pl.semaphore_wait(known_sem.at[ALL], 1)

    @pl.when(jnp.logical_not(is_late))
    def _():
        give(HUB - 1)

    piece_recv[gy] = piece_send[pl.ds(pl.multiple_of(gy * SIDE, SIDE), SIDE), :]

    view_of = lax.div(lane, 4 * SIDE)
    kind_of = lax.rem(lax.div(lane, SIDE), 4)
    ranks = []
    for group in range(GROUPS):
        rank = jnp.full((SIDE, DEPTH), order_s[0, group], jnp.int32)
        for view in range(1, VIEWS):
            rank = jnp.where(view_of == view, order_s[view, group], rank)
        ranks.append(rank)
    is_depth = kind_of == 3

    def arrive(number, tiles):
        slots = piece_recv.at[pl.ds(0, tiles)]
        pltpu.make_async_remote_copy(
            src_ref=slots,
            dst_ref=slots,
            send_sem=local_sem.at[6],
            recv_sem=piece_recv_sem.at[number],
            device_id=(gx, gy_lo),
            device_id_type=MESH,
        ).wait_recv()

    depths, fronts = {}, {}

    def place(group):
        value = jnp.where(is_depth, piece_recv[group], 0.0)
        value = value + pltpu.roll(value, DEPTH - SIDE, 1)
        depths[group] = value + pltpu.roll(value, DEPTH - 2 * SIDE, 1)
        total = jnp.zeros((SIDE, DEPTH), F32)
        for other in fronts:
            before = ranks[other] < ranks[group]
            total = total + jnp.where(before, depths[other], 0.0)
            fronts[other] = fronts[other] + jnp.where(before, 0.0, depths[group])
        fronts[group] = total

    for number, groups, tiles in ((0, range(LATE, GROUPS), GROUPS - LATE), (1, range(LATE), LATE)):
        own_late = among_late == number

        @pl.when(own_late)
        def _():
            arrive(number, tiles - 1)

        @pl.when(jnp.logical_not(own_late))
        def _():
            arrive(number, tiles)

        for group in groups:
            place(group)
    color = sum(jnp.exp(-fronts[group]) * piece_recv[group] for group in range(GROUPS))
    opaque = 1.0 - jnp.exp(-sum(depths.values()))
    image_v[...] = jnp.transpose(jnp.where(is_depth, opaque, color))
    for present, copy in x_waits + y_waits:

        @pl.when(present)
        def _():
            copy.wait_send()

    sent = piece_recv.at[pl.ds(0, GROUPS - 1)]
    pltpu.make_async_remote_copy(
        src_ref=sent,
        dst_ref=sent,
        send_sem=local_sem.at[6],
        recv_sem=piece_recv_sem.at[0],
        device_id=(gx, gy_lo),
        device_id_type=MESH,
    ).wait_send()


def put_out(head_v, temp_v, image_v, head_out, temp_out, image_out, sem):
    copies = [
        pltpu.make_async_copy(src, dst, sem.at[number])
        for number, (src, dst) in enumerate(
            ((image_v, image_out), (head_v, head_out), (temp_v, temp_out))
        )
    ]
    for copy in copies:
        copy.start()
    for copy in copies:
        copy.wait()


def shards(head, temp, category, ice, *params):
    gx_count, gy_count = lax.axis_size("gx"), lax.axis_size("gy")
    rows = SIDE * SIDE
    flat = [a.reshape(rows, DEPTH) for a in (head, temp, category, ice)]
    vmem = pltpu.VMEM
    dma = pltpu.SemaphoreType.DMA
    shapes = ((rows, DEPTH), (rows, DEPTH), (DEPTH, SIDE))
    results = pl.pallas_call(
        functools.partial(kernel, gx_count, gy_count),
        out_shape=tuple(pltpu.VMEM(shape, F32) for shape in shapes),
        in_specs=[pl.BlockSpec(memory_space=pl.ANY)] * 10,
        out_specs=[pl.BlockSpec(memory_space=pltpu.VMEM)] * 3,
        scratch_shapes=[
            vmem((rows, DEPTH), F32),
            vmem((rows, DEPTH), F32),
            vmem((rows, DEPTH), jnp.int32),
            vmem((rows, DEPTH), jnp.int32),
            pltpu.SMEM((SOILS,), F32),
            pltpu.SMEM((SOILS,), F32),
            pltpu.SMEM((VIEWS,), F32),
            pltpu.SMEM((3,), F32),
            pltpu.SMEM((3,), F32),
            pltpu.SMEM((VIEWS, GROUPS), jnp.int32),
            vmem((2, 6 * SIDE, DEPTH), F32),
            vmem((2, 6 * SIDE, DEPTH), F32),
            vmem((2, 6 * SIDE, DEPTH), F32),
            vmem((2, 6 * SIDE, DEPTH), F32),
            vmem((2, 2, 4, DEPTH), F32),
            vmem((2, 2, 4, DEPTH), F32),
            vmem((6, 3, SIDE, DEPTH), F32),
            vmem((DEPTH, DEPTH), F32),
            vmem((GROUPS, SIDE, DEPTH), F32),
            dma((12,)),
            dma((8,)),
            pltpu.SemaphoreType.REGULAR((6,)),
            dma((2,)),
        ],
        compiler_params=pltpu.CompilerParams(collective_id=0, has_side_effects=True),
        name="step_and_view",
    )(*flat, *params)
    head, temp, image = pl.pallas_call(
        put_out,
        out_shape=tuple(jax.ShapeDtypeStruct(shape, F32) for shape in shapes),
        in_specs=[pl.BlockSpec(memory_space=pltpu.VMEM)] * 3,
        out_specs=[pl.BlockSpec(memory_space=pl.ANY)] * 3,
        scratch_shapes=[dma((3,))],
        name="put_out",
    )(*(pltpu.with_memory_space_constraint(r, pltpu.VMEM) for r in results))
    shape = (SIDE, SIDE, DEPTH)
    return head.reshape(shape), temp.reshape(shape), image.reshape(VIEWS, 4, SIDE, SIDE)


def solution(mesh):
    block = P("gx", "gy", None)
    return jax.shard_map(
        shards,
        mesh=mesh,
        in_specs=(block,) * 4 + (P(),) * 6,
        out_specs=(block, block, P(None, None, "gx", "gy")),
        check_vma=False,
    )
```

```python
import functools

import jax
import jax.numpy as jnp
from jax import lax
from jax.experimental import pallas as pl
from jax.experimental.pallas import tpu as pltpu
from jax.sharding import PartitionSpec as P

MESH = pl.DeviceIdType.MESH
SOILS = 12
VIEWS = 4
SIDE = 8
DEPTH = 128
GROUPS = 16
DIFFUSE = 0.12
HUB = 1
LATE = 2
BEFORE, CROSS, BELOW, DIAGONAL, MOST, ALL = range(6)
F32 = jnp.float32


def lookup(category, table):
    total = jnp.full(category.shape, table[0], F32)
    for number in range(1, SOILS):
        total = jnp.where(category == number, table[number], total)
    return total


def conductivity(head, temp, ks, alpha, ice):
    return ks * jnp.exp(alpha * jnp.minimum(head, 0.0) + 2.0 * ice * (jnp.tanh(temp) - 1.0))


def face(k_a, h_a, k_b, h_b):
    return (k_a + k_b) * (h_b - h_a)


def vertical(head, temp, conduct, lane):
    inner_lo, inner_hi = lane > 0, lane < DEPTH - 1
    above, conduct_above = (pltpu.roll(a, DEPTH - 1, 1) for a in (head, conduct))
    below, conduct_below = (pltpu.roll(a, 1, 1) for a in (head, conduct))
    change = jnp.where(inner_hi, (conduct + conduct_above) * (above - head + 1.0), 0.0) - jnp.where(
        inner_lo, (conduct + conduct_below) * (head - below + 1.0), 0.0
    )
    warm = jnp.where(inner_hi, pltpu.roll(temp, DEPTH - 1, 1), 0.0) + jnp.where(
        inner_lo, pltpu.roll(temp, 1, 1), 0.0
    )
    return change, warm


def kernel(
    gx_count,
    gy_count,
    head_in,
    temp_in,
    cat_in,
    ice_in,
    ks_in,
    alpha_in,
    skew_in,
    steep_in,
    mid_in,
    order_in,
    head_v,
    temp_v,
    image_v,
    head_a,
    temp_a,
    cat_a,
    ice_a,
    ks_s,
    alpha_s,
    skew_s,
    steep_s,
    mid_s,
    order_s,
    y_send,
    y_recv,
    x_send,
    x_recv,
    c_send,
    c_recv,
    ghost,
    piece_send,
    piece_recv,
    local_sem,
    halo_recv_sem,
    known_sem,
    piece_recv_sem,
):
    gx, gy = lax.axis_index("gx"), lax.axis_index("gy")
    gx_lo, gx_hi = lax.rem(gx + gx_count - 1, gx_count), lax.rem(gx + 1, gx_count)
    gy_lo, gy_hi = lax.rem(gy + gy_count - 1, gy_count), lax.rem(gy + 1, gy_count)

    loads = [
        pltpu.make_async_copy(src, dst, local_sem.at[number])
        for number, (src, dst) in enumerate(
            ((head_in, head_a), (temp_in, temp_a), (cat_in, cat_a), (ice_in, ice_a))
        )
    ]
    params = [
        pltpu.make_async_copy(src, dst, local_sem.at[4 + number])
        for number, (src, dst) in enumerate(
            (
                (ks_in, ks_s),
                (alpha_in, alpha_s),
                (skew_in, skew_s),
                (steep_in, steep_s),
                (mid_in, mid_s),
                (order_in, order_s),
            )
        )
    ]
    for copy in params[:2] + loads + params[2:]:
        copy.start()

    px, py = lax.div(gy, 4), lax.rem(gy, 4)
    shifts = sorted(
        ((dx, dy) for dx in range(4) for dy in range(4) if (dx, dy) != (0, 0)),
        key=lambda d: -(min(d[0], 4 - d[0]) + min(d[1], 4 - d[1])),
    )
    peers = [lax.rem(px + dx, 4) * 4 + lax.rem(py + dy, 4) for dx, dy in shifts]

    has_x = (gx > 0, gx < gx_count - 1)
    has_y = (gy > 0, gy < gy_count - 1)
    x_at, y_at = (gx_lo, gx_hi), (gy_lo, gy_hi)
    both = [[jnp.logical_and(has_x[a], has_y[b]) for b in range(2)] for a in range(2)]
    is_hub = gy == HUB
    is_late = gy == HUB - 1
    far_from_hub = jnp.abs(gy - HUB) > 1

    barrier = pltpu.get_barrier_semaphore()

    def greet(device):
        pl.semaphore_signal(barrier, inc=1, device_id=device, device_id_type=MESH)

    def tell(number, device):
        pl.semaphore_signal(known_sem.at[number], inc=1, device_id=device, device_id_type=MESH)

    for a in range(2):

        @pl.when(both[a][0])
        def _():
            greet((x_at[a], gy_lo))

    @pl.when(has_y[0])
    def _():
        greet((gx, gy_lo))

    @pl.when(has_x[0])
    def _():
        greet((gx_lo, gy))

    @pl.when(far_from_hub)
    def _():
        greet((gx, HUB))

    def one(flag):
        return flag.astype(jnp.int32)

    x_sides = one(has_x[0]) + one(has_x[1])
    gathered = jnp.where(is_hub, gy_count - 3, 0)
    awaited = gathered + one(has_x[1]) + one(has_y[1]) * (1 + x_sides)

    @pl.when(awaited > 0)
    def _():
        pl.semaphore_wait(barrier, awaited)

    for a in range(2):

        @pl.when(both[a][1])
        def _():
            tell((CROSS, DIAGONAL)[a], (x_at[a], gy_hi))

    @pl.when(has_y[1])
    def _():
        tell(BELOW, (gx, gy_hi))

    @pl.when(has_x[1])
    def _():
        tell(BEFORE, (gx_hi, gy))

    @pl.when(is_hub)
    def _():
        for peer in peers:

            @pl.when(peer != HUB - 1)
            def _():
                tell(MOST, (gx, peer))

    row = lax.broadcasted_iota(jnp.int32, (SIDE, DEPTH), 0)
    lane = lax.broadcasted_iota(jnp.int32, (SIDE, DEPTH), 1)
    first, last = row == 0, row == SIDE - 1

    for copy in params[:2] + loads:
        copy.wait()

    def across(ref, y):
        return ref[pl.ds(y, SIDE, stride=SIDE), :]

    def tile(ref, x):
        return ref[pl.ds(x * SIDE, SIDE), :]

    head, temp, category, ice, ks, alpha, conduct = ({} for _ in range(7))

    def own(y):
        head[y], temp[y], category[y] = across(head_a, y), across(temp_a, y), across(cat_a, y)
        ice[y] = across(ice_a, y).astype(F32)
        ks[y], alpha[y] = lookup(category[y], ks_s), lookup(category[y], alpha_s)
        conduct[y] = conductivity(head[y], temp[y], ks[y], alpha[y], ice[y])

    def remote(src, dst, mine, theirs, device):
        return pltpu.make_async_remote_copy(
            src_ref=src,
            dst_ref=dst,
            send_sem=local_sem.at[(0, 1, 2, 3, 4, 5, 10, 11)[mine]],
            recv_sem=halo_recv_sem.at[theirs],
            device_id=device,
            device_id_type=MESH,
        )

    def y_copy(b):
        return remote(y_send.at[b], y_recv.at[1 - b], b, 1 - b, (gx, y_at[b]))

    def x_copy(a):
        return remote(x_send.at[a], x_recv.at[1 - a], 2 + a, 3 - a, (x_at[a], gy))

    def c_copy(a, b):
        slot = 4 + 2 * a + b
        return remote(
            c_send.at[a, b], c_recv.at[1 - a, 1 - b], slot, 11 - slot, (x_at[a], y_at[b])
        )

    def send(present, copy, *known):
        @pl.when(present)
        def _():
            for number in known:
                pl.semaphore_wait(known_sem.at[number], 1)
            copy.start()

    def stage_y(side):
        near, far = ((0, 1), (SIDE - 1, SIDE - 2))[side]
        own(near)
        own(far)
        parts = (
            head[near],
            temp[near],
            category[near].astype(F32),
            ice[near],
            face(conduct[near], head[near], conduct[far], head[far]),
            temp[far],
        )
        for number, part in enumerate(parts):
            y_send[side, pl.ds(number * SIDE, SIDE), :] = part
        for a, x in enumerate((0, SIDE - 1)):
            for field, part in enumerate((head[near], temp[near], conduct[near], conduct[near])):
                c_send[a, side, pl.ds(field, 1), :] = part[x : x + 1, :]

    stage_y(1)
    for a in range(2):
        send(both[a][1], c_copy(a, 1))
    send(has_y[1], y_copy(1))

    edge = {}
    for x in (0, 1, SIDE - 2, SIDE - 1):
        h, t, c = tile(head_a, x), tile(temp_a, x), tile(cat_a, x)
        i = tile(ice_a, x).astype(F32)
        k = conductivity(h, t, lookup(c, ks_s), lookup(c, alpha_s), i)
        edge[x] = (h, t, c.astype(F32), i, k)
    for side, (near, far) in enumerate(((0, 1), (SIDE - 1, SIDE - 2))):
        inner, outer = edge[far], edge[near]
        parts = (*outer[:4], face(outer[4], outer[0], inner[4], inner[0]), inner[1])
        for number, part in enumerate(parts):
            x_send[side, pl.ds(number * SIDE, SIDE), :] = part
    send(has_x[1], x_copy(1))
    stage_y(0)
    send(has_x[0], x_copy(0), BEFORE)
    send(both[1][0], c_copy(1, 0), CROSS)
    send(has_y[0], y_copy(0), BELOW)

    @pl.when(is_hub)
    def _():
        for peer in peers:
            tell(ALL, (gx, peer))

    send(both[0][0], c_copy(0, 0), DIAGONAL)

    for copy in params[2:]:
        copy.wait()

    x_open = (jnp.logical_or(row > 0, has_x[0]), jnp.logical_or(row < SIDE - 1, has_x[1]))
    y_open = (jnp.logical_or(row > 0, has_y[0]), jnp.logical_or(row < SIDE - 1, has_y[1]))

    for y in range(2, SIDE - 2):
        own(y)

    def arrived(a, b):
        slot = 4 + 2 * a + b
        return remote(c_send.at[a, b], c_recv.at[a, b], slot, slot, (gx, gy_lo))

    x_waits = [
        (has_x[a], remote(x_send.at[a], x_recv.at[a], 2 + a, 2 + a, (gx, gy_lo)))
        for a in range(2)
    ]
    y_waits = [(both[a][b], arrived(a, b)) for a in range(2) for b in range(2)]
    y_waits += [
        (has_y[b], remote(y_send.at[b], y_recv.at[b], b, b, (gx, gy_lo))) for b in range(2)
    ]

    def receive(waits):
        for present, copy in waits:

            @pl.when(present)
            def _():
                copy.wait_recv()

    def along_rows(value, before, after):
        return (
            jnp.where(first, before, pltpu.roll(value, 1, 0)),
            jnp.where(last, after, pltpu.roll(value, SIDE - 1, 0)),
        )

    def change_rows(head_, conduct_, temp_, ends, opened):
        (h_lo, t_lo, k_lo), (h_hi, t_hi, k_hi) = ends
        heads = along_rows(head_, h_lo, h_hi)
        temps = along_rows(temp_, t_lo, t_hi)
        conducts = along_rows(conduct_, k_lo, k_hi)
        total = sum(
            jnp.where(opened[s], (conduct_ + conducts[s]) * (heads[s] - head_), 0.0)
            for s in range(2)
        )
        return total, temps[0] + temps[1]

    def y_part(side, number):
        return y_recv[side, pl.ds(number * SIDE, SIDE), :]

    def x_part(side, number):
        return x_recv[side, pl.ds(number * SIDE, SIDE), :]

    def warm_if(present, value):
        return jnp.where(present, value, 0.0)

    def corner(xs, ys):
        return (
            c_recv[xs, ys, pl.ds(0, 1), :],
            warm_if(jnp.logical_and(has_x[xs], has_y[ys]), c_recv[xs, ys, pl.ds(1, 1), :]),
            c_recv[xs, ys, pl.ds(2, 1), :],
        )

    def read_ghost(part_of, side, present):
        h, t, c, i = (part_of(side, number) for number in range(4))
        k_s, a = lookup(c, ks_s), lookup(c, alpha_s)
        far = tuple(part_of(side, number) for number in range(4, 6))
        return h, warm_if(present, t), conductivity(h, t, k_s, a, i), k_s, a, i, far

    def step(h, t, change, warm):
        return h + 0.5 * change, t + DIFFUSE * (warm - 6.0 * t)

    def ghost_base(cell, inner):
        h, t, k, far = cell[0], cell[1], cell[2], cell[6]
        change, warm = vertical(h, t, k, lane)
        change = change + far[0] + face(k, h, inner[2], inner[0])
        return change, warm + far[1] + inner[1]

    def ghost_step(cell, base, ends, opened, present):
        h, t, k, k_s, a, i, _ = cell
        rows, rows_warm = change_rows(h, k, t, ends, opened)
        h, t = step(h, t, base[0] + rows, base[1] + rows_warm)
        return h, warm_if(present, t), conductivity(h, t, k_s, a, i)

    def keep(slot, cells):
        for side in range(2):
            for field in range(3):
                ghost[slot + side, field] = cells[side][field]

    def base_of(y, h, t, k, slot):
        ends = tuple(
            tuple(ghost[slot + side, field, pl.ds(y, 1), :] for field in range(3))
            for side in range(2)
        )
        change, warm = vertical(h[y], t[y], k[y], lane)
        rows, rows_warm = change_rows(h[y], k[y], t[y], ends, x_open)
        return change + rows, warm + rows_warm

    def plane_step(y, h, t, k, base, faces):
        for edge_ in (y, y + 1):
            if edge_ not in faces:
                value = face(k[edge_ - 1], h[edge_ - 1], k[edge_], h[edge_])
                if edge_ in (0, SIDE):
                    value = jnp.where(has_y[edge_ // SIDE], value, 0.0)
                faces[edge_] = value
        return step(
            h[y],
            t[y],
            base[0] + faces[y + 1] - faces[y],
            base[1] + t[y - 1] + t[y + 1],
        )

    planes_all = gy_count * SIDE

    def view_planes(view, planes, theta):
        clear = depth = None
        sums = [None] * 3
        for y in planes:
            shift = skew_s[view] * ((gy * SIDE + y).astype(F32) - 0.5 * planes_all)
            wrapped = shift - DEPTH * jnp.floor(shift * (1.0 / DEPTH))
            base = jnp.floor(wrapped)
            part = wrapped - base
            turn = lax.rem(2 * DEPTH - base.astype(jnp.int32), DEPTH)
            lower = pltpu.roll(theta[y], turn, 1)
            upper = pltpu.roll(theta[y], lax.rem(turn + DEPTH - 1, DEPTH), 1)
            sample = (1.0 - part) * lower + part * upper
            optical = sample * (8.0 / planes_all)
            passed = jnp.exp(-optical)
            after = passed if clear is None else clear * passed
            weight = (1.0 if clear is None else clear) - after
            clear = after
            depth = optical if depth is None else depth + optical
            for color in range(3):
                term = weight * jnp.tanh((0.5 * steep_s[color]) * (sample - mid_s[color]))
                sums[color] = term if sums[color] is None else sums[color] + term
        return clear, sums, depth

    theta = {}

    def finish(y, h, t):
        head_v[pl.ds(y, SIDE, stride=SIDE), :] = h
        temp_v[pl.ds(y, SIDE, stride=SIDE), :] = t
        theta[y] = 0.05 + 0.4 * jnp.exp(0.8 * jnp.minimum(h, 0.0))

    receive(x_waits)
    x_ghost = [read_ghost(x_part, side, has_x[side]) for side in range(2)]
    keep(0, x_ghost)
    bases = [base_of(y, head, temp, conduct, 0) for y in range(SIDE)]
    faces, head_1, temp_1, conduct_1 = {}, {}, {}, {}

    def first_step(y):
        head_1[y], temp_1[y] = plane_step(y, head, temp, conduct, bases[y], faces)
        conduct_1[y] = conductivity(head_1[y], temp_1[y], ks[y], alpha[y], ice[y])

    for y in range(1, SIDE - 1):
        first_step(y)
    x_bases = [
        ghost_base(x_ghost[side], (edge[x][0], edge[x][1], edge[x][4]))
        for side, x in ((0, 0), (1, SIDE - 1))
    ]
    nothing = jnp.zeros((1, DEPTH), F32)
    keep(
        2,
        [
            ghost_step(x_ghost[side], x_bases[side], ((nothing,) * 3,) * 2, y_open, has_x[side])
            for side in range(2)
        ],
    )
    bases_1 = {y: base_of(y, head_1, temp_1, conduct_1, 2) for y in range(1, SIDE - 1)}
    faces_1 = {}
    middle = range(2, SIDE - 2)
    for y in middle:
        finish(y, *plane_step(y, head_1, temp_1, conduct_1, bases_1[y], faces_1))
    middles = [view_planes(view, middle, theta) for view in range(VIEWS)]

    receive(y_waits)
    y_ghost = [read_ghost(y_part, side, has_y[side]) for side in range(2)]
    for side, y in ((0, -1), (1, SIDE)):
        head[y], temp[y], conduct[y] = y_ghost[side][:3]
    for y in (0, SIDE - 1):
        first_step(y)
    for side, y, out in ((0, 0, -1), (1, SIDE - 1, SIDE)):
        head_1[out], temp_1[out], conduct_1[out] = ghost_step(
            y_ghost[side],
            ghost_base(y_ghost[side], (head[y], temp[y], conduct[y])),
            (corner(0, side), corner(1, side)),
            x_open,
            has_y[side],
        )
    keep(
        4,
        [
            ghost_step(
                x_ghost[side],
                x_bases[side],
                (corner(side, 0), corner(side, 1)),
                y_open,
                has_x[side],
            )
            for side in range(2)
        ],
    )
    for y in (0, SIDE - 1):
        bases_1[y] = base_of(y, head_1, temp_1, conduct_1, 4)
    for y in (0, 1, SIDE - 2, SIDE - 1):
        finish(y, *plane_step(y, head_1, temp_1, conduct_1, bases_1[y], faces_1))

    layers = []
    for view in range(VIEWS):
        clear_a, sums_a, depth_a = view_planes(view, (0, 1), theta)
        clear_b, sums_b, depth_b = middles[view]
        clear_c, sums_c, depth_c = view_planes(view, (SIDE - 2, SIDE - 1), theta)
        opaque = 1.0 - clear_a * (clear_b * clear_c)
        for color in range(3):
            total = sums_a[color] + clear_a * (sums_b[color] + clear_b * sums_c[color])
            layers.append(0.5 * (opaque + total))
        layers.append(depth_a + depth_b + depth_c)
    piece_send[...] = jnp.transpose(jnp.concatenate(layers, 0))

    among_late = jnp.where(gy < LATE, 1, 0)

    def exchange(src, dst, device):
        return pltpu.make_async_remote_copy(
            src_ref=src,
            dst_ref=dst,
            send_sem=local_sem.at[6],
            recv_sem=piece_recv_sem.at[among_late],
            device_id=device,
            device_id_type=MESH,
        )

    plain = jnp.logical_not(jnp.logical_or(is_hub, is_late))

    def give(peer):
        exchange(
            piece_send.at[pl.ds(pl.multiple_of(peer * SIDE, SIDE), SIDE)],
            piece_recv.at[gy],
            (gx, peer),
        ).start()

    @pl.when(plain)
    def _():
        pl.semaphore_wait(known_sem.at[MOST], 1)

    @pl.when(is_late)
    def _():
        pl.semaphore_wait(known_sem.at[ALL], 1)

    @pl.when(is_hub)
    def _():
        give(HUB - 1)

    soon = [(2, 3), (1, 3), (3, 3), (2, 0), (1, 0), (3, 0)]
    for dx, dy in soon + [d for d in shifts if d not in soon]:
        peer = lax.rem(px + dx, 4) * 4 + lax.rem(py + dy, 4)

        @pl.when(peer != HUB - 1)
        def _():
            give(peer)

    @pl.when(plain)
    def _():
        pl.semaphore_wait(known_sem.at[ALL], 1)
        give(HUB - 1)

    piece_recv[gy] = piece_send[pl.ds(pl.multiple_of(gy * SIDE, SIDE), SIDE), :]

    view_of = lax.div(lane, 4 * SIDE)
    kind_of = lax.rem(lax.div(lane, SIDE), 4)
    ranks = []
    for group in range(GROUPS):
        rank = jnp.full((SIDE, DEPTH), order_s[0, group], jnp.int32)
        for view in range(1, VIEWS):
            rank = jnp.where(view_of == view, order_s[view, group], rank)
        ranks.append(rank)
    is_depth = kind_of == 3

    def arrive(number, tiles):
        slots = piece_recv.at[pl.ds(0, tiles)]
        pltpu.make_async_remote_copy(
            src_ref=slots,
            dst_ref=slots,
            send_sem=local_sem.at[6],
            recv_sem=piece_recv_sem.at[number],
            device_id=(gx, gy_lo),
            device_id_type=MESH,
        ).wait_recv()

    depths, fronts = {}, {}

    def place(group):
        value = jnp.where(is_depth, piece_recv[group], 0.0)
        value = value + pltpu.roll(value, DEPTH - SIDE, 1)
        depths[group] = value + pltpu.roll(value, DEPTH - 2 * SIDE, 1)
        total = jnp.zeros((SIDE, DEPTH), F32)
        for other in fronts:
            before = ranks[other] < ranks[group]
            total = total + jnp.where(before, depths[other], 0.0)
            fronts[other] = fronts[other] + jnp.where(before, 0.0, depths[group])
        fronts[group] = total

    for number, groups, tiles in ((0, range(LATE, GROUPS), GROUPS - LATE), (1, range(LATE), LATE)):
        own_late = among_late == number

        @pl.when(own_late)
        def _():
            arrive(number, tiles - 1)

        @pl.when(jnp.logical_not(own_late))
        def _():
            arrive(number, tiles)

        for group in groups:
            place(group)
    color = sum(jnp.exp(-fronts[group]) * piece_recv[group] for group in range(GROUPS))
    opaque = 1.0 - jnp.exp(-sum(depths.values()))
    image_v[...] = jnp.transpose(jnp.where(is_depth, opaque, color))
    for present, copy in x_waits + y_waits:

        @pl.when(present)
        def _():
            copy.wait_send()

    sent = piece_recv.at[pl.ds(0, GROUPS - 1)]
    pltpu.make_async_remote_copy(
        src_ref=sent,
        dst_ref=sent,
        send_sem=local_sem.at[6],
        recv_sem=piece_recv_sem.at[0],
        device_id=(gx, gy_lo),
        device_id_type=MESH,
    ).wait_send()


def put_out(head_v, temp_v, image_v, head_out, temp_out, image_out, sem):
    copies = [
        pltpu.make_async_copy(src, dst, sem.at[number])
        for number, (src, dst) in enumerate(
            ((image_v, image_out), (head_v, head_out), (temp_v, temp_out))
        )
    ]
    for copy in copies:
        copy.start()
    for copy in copies:
        copy.wait()


def shards(head, temp, category, ice, *params):
    gx_count, gy_count = lax.axis_size("gx"), lax.axis_size("gy")
    rows = SIDE * SIDE
    flat = [a.reshape(rows, DEPTH) for a in (head, temp, category, ice)]
    vmem = pltpu.VMEM
    dma = pltpu.SemaphoreType.DMA
    shapes = ((rows, DEPTH), (rows, DEPTH), (DEPTH, SIDE))
    results = pl.pallas_call(
        functools.partial(kernel, gx_count, gy_count),
        out_shape=tuple(pltpu.VMEM(shape, F32) for shape in shapes),
        in_specs=[pl.BlockSpec(memory_space=pl.ANY)] * 10,
        out_specs=[pl.BlockSpec(memory_space=pltpu.VMEM)] * 3,
        scratch_shapes=[
            vmem((rows, DEPTH), F32),
            vmem((rows, DEPTH), F32),
            vmem((rows, DEPTH), jnp.int32),
            vmem((rows, DEPTH), jnp.int32),
            pltpu.SMEM((SOILS,), F32),
            pltpu.SMEM((SOILS,), F32),
            pltpu.SMEM((VIEWS,), F32),
            pltpu.SMEM((3,), F32),
            pltpu.SMEM((3,), F32),
            pltpu.SMEM((VIEWS, GROUPS), jnp.int32),
            vmem((2, 6 * SIDE, DEPTH), F32),
            vmem((2, 6 * SIDE, DEPTH), F32),
            vmem((2, 6 * SIDE, DEPTH), F32),
            vmem((2, 6 * SIDE, DEPTH), F32),
            vmem((2, 2, 4, DEPTH), F32),
            vmem((2, 2, 4, DEPTH), F32),
            vmem((6, 3, SIDE, DEPTH), F32),
            vmem((DEPTH, DEPTH), F32),
            vmem((GROUPS, SIDE, DEPTH), F32),
            dma((12,)),
            dma((8,)),
            pltpu.SemaphoreType.REGULAR((6,)),
            dma((2,)),
        ],
        compiler_params=pltpu.CompilerParams(collective_id=0, has_side_effects=True),
        name="step_and_view",
    )(*flat, *params)
    head, temp, image = pl.pallas_call(
        put_out,
        out_shape=tuple(jax.ShapeDtypeStruct(shape, F32) for shape in shapes),
        in_specs=[pl.BlockSpec(memory_space=pltpu.VMEM)] * 3,
        out_specs=[pl.BlockSpec(memory_space=pl.ANY)] * 3,
        scratch_shapes=[dma((3,))],
        name="put_out",
    )(*(pltpu.with_memory_space_constraint(r, pltpu.VMEM) for r in results))
    shape = (SIDE, SIDE, DEPTH)
    return head.reshape(shape), temp.reshape(shape), image.reshape(VIEWS, 4, SIDE, SIDE)


def solution(mesh):
    block = P("gx", "gy", None)
    return jax.shard_map(
        shards,
        mesh=mesh,
        in_specs=(block,) * 4 + (P(),) * 6,
        out_specs=(block, block, P(None, None, "gx", "gy")),
        check_vma=False,
    )
```

```python
import functools

import jax
import jax.numpy as jnp
from jax import lax
from jax.experimental import pallas as pl
from jax.experimental.pallas import tpu as pltpu
from jax.sharding import PartitionSpec as P

MESH = pl.DeviceIdType.MESH
SOILS = 12
VIEWS = 4
SIDE = 8
DEPTH = 128
GROUPS = 16
DIFFUSE = 0.12
HUB = 1
LATE = 2
BEFORE, CROSS, BELOW, DIAGONAL, MOST, ALL = range(6)
F32 = jnp.float32


def lookup(category, table):
    half = SOILS // 2
    parts = []
    for start in (0, half):
        total = jnp.full(category.shape, table[start], F32)
        for number in range(start + 1, start + half):
            total = jnp.where(category == number, table[number], total)
        parts.append(total)
    return jnp.where(category < half, *parts)


def conductivity(head, temp, ks, alpha, ice):
    return ks * jnp.exp(alpha * jnp.minimum(head, 0.0) + 2.0 * ice * (jnp.tanh(temp) - 1.0))


def face(k_a, h_a, k_b, h_b):
    return (k_a + k_b) * (h_b - h_a)


def vertical(head, temp, conduct, lane):
    inner_lo, inner_hi = lane > 0, lane < DEPTH - 1
    above, conduct_above = (pltpu.roll(a, DEPTH - 1, 1) for a in (head, conduct))
    below, conduct_below = (pltpu.roll(a, 1, 1) for a in (head, conduct))
    change = jnp.where(inner_hi, (conduct + conduct_above) * (above - head + 1.0), 0.0) - jnp.where(
        inner_lo, (conduct + conduct_below) * (head - below + 1.0), 0.0
    )
    warm = jnp.where(inner_hi, pltpu.roll(temp, DEPTH - 1, 1), 0.0) + jnp.where(
        inner_lo, pltpu.roll(temp, 1, 1), 0.0
    )
    return change, warm


def kernel(
    gx_count,
    gy_count,
    head_in,
    temp_in,
    cat_in,
    ice_in,
    ks_in,
    alpha_in,
    skew_in,
    steep_in,
    mid_in,
    order_in,
    head_v,
    temp_v,
    image_v,
    head_a,
    temp_a,
    cat_a,
    ice_a,
    ks_s,
    alpha_s,
    skew_s,
    steep_s,
    mid_s,
    order_s,
    y_send,
    y_recv,
    x_send,
    x_recv,
    c_send,
    c_recv,
    ghost,
    piece_send,
    piece_recv,
    local_sem,
    halo_recv_sem,
    known_sem,
    piece_recv_sem,
):
    gx, gy = lax.axis_index("gx"), lax.axis_index("gy")
    gx_lo, gx_hi = lax.rem(gx + gx_count - 1, gx_count), lax.rem(gx + 1, gx_count)
    gy_lo, gy_hi = lax.rem(gy + gy_count - 1, gy_count), lax.rem(gy + 1, gy_count)

    loads = [
        pltpu.make_async_copy(src, dst, local_sem.at[number])
        for number, (src, dst) in enumerate(
            ((head_in, head_a), (temp_in, temp_a), (cat_in, cat_a), (ice_in, ice_a))
        )
    ]
    params = [
        pltpu.make_async_copy(src, dst, local_sem.at[4 + number])
        for number, (src, dst) in enumerate(
            (
                (ks_in, ks_s),
                (alpha_in, alpha_s),
                (skew_in, skew_s),
                (steep_in, steep_s),
                (mid_in, mid_s),
                (order_in, order_s),
            )
        )
    ]
    for copy in params[:2] + loads + params[2:]:
        copy.start()

    px, py = lax.div(gy, 4), lax.rem(gy, 4)
    shifts = sorted(
        ((dx, dy) for dx in range(4) for dy in range(4) if (dx, dy) != (0, 0)),
        key=lambda d: -(min(d[0], 4 - d[0]) + min(d[1], 4 - d[1])),
    )
    peers = [lax.rem(px + dx, 4) * 4 + lax.rem(py + dy, 4) for dx, dy in shifts]

    has_x = (gx > 0, gx < gx_count - 1)
    has_y = (gy > 0, gy < gy_count - 1)
    x_at, y_at = (gx_lo, gx_hi), (gy_lo, gy_hi)
    both = [[jnp.logical_and(has_x[a], has_y[b]) for b in range(2)] for a in range(2)]
    is_hub = gy == HUB
    is_late = gy == HUB - 1
    far_from_hub = jnp.abs(gy - HUB) > 1

    barrier = pltpu.get_barrier_semaphore()

    def greet(device):
        pl.semaphore_signal(barrier, inc=1, device_id=device, device_id_type=MESH)

    def tell(number, device):
        pl.semaphore_signal(known_sem.at[number], inc=1, device_id=device, device_id_type=MESH)

    for a in range(2):

        @pl.when(both[a][0])
        def _():
            greet((x_at[a], gy_lo))

    @pl.when(has_y[0])
    def _():
        greet((gx, gy_lo))

    @pl.when(has_x[0])
    def _():
        greet((gx_lo, gy))

    @pl.when(far_from_hub)
    def _():
        greet((gx, HUB))

    def one(flag):
        return flag.astype(jnp.int32)

    x_sides = one(has_x[0]) + one(has_x[1])
    gathered = jnp.where(is_hub, gy_count - 3, 0)
    awaited = gathered + one(has_x[1]) + one(has_y[1]) * (1 + x_sides)

    @pl.when(awaited > 0)
    def _():
        pl.semaphore_wait(barrier, awaited)

    for a in range(2):

        @pl.when(both[a][1])
        def _():
            tell((CROSS, DIAGONAL)[a], (x_at[a], gy_hi))

    @pl.when(has_y[1])
    def _():
        tell(BELOW, (gx, gy_hi))

    @pl.when(has_x[1])
    def _():
        tell(BEFORE, (gx_hi, gy))

    @pl.when(is_hub)
    def _():
        for peer in peers:

            @pl.when(peer != HUB - 1)
            def _():
                tell(MOST, (gx, peer))

    row = lax.broadcasted_iota(jnp.int32, (SIDE, DEPTH), 0)
    lane = lax.broadcasted_iota(jnp.int32, (SIDE, DEPTH), 1)
    first, last = row == 0, row == SIDE - 1

    for copy in params[:2] + loads:
        copy.wait()

    def across(ref, y):
        return ref[pl.ds(y, SIDE, stride=SIDE), :]

    def tile(ref, x):
        return ref[pl.ds(x * SIDE, SIDE), :]

    head, temp, category, ice, ks, alpha, conduct = ({} for _ in range(7))

    def own(y):
        head[y], temp[y], category[y] = across(head_a, y), across(temp_a, y), across(cat_a, y)
        ice[y] = across(ice_a, y).astype(F32)
        ks[y], alpha[y] = lookup(category[y], ks_s), lookup(category[y], alpha_s)
        conduct[y] = conductivity(head[y], temp[y], ks[y], alpha[y], ice[y])

    def remote(src, dst, mine, theirs, device):
        return pltpu.make_async_remote_copy(
            src_ref=src,
            dst_ref=dst,
            send_sem=local_sem.at[(0, 1, 2, 3, 4, 5, 10, 11)[mine]],
            recv_sem=halo_recv_sem.at[theirs],
            device_id=device,
            device_id_type=MESH,
        )

    def y_copy(b):
        return remote(y_send.at[b], y_recv.at[1 - b], b, 1 - b, (gx, y_at[b]))

    def x_copy(a):
        return remote(x_send.at[a], x_recv.at[1 - a], 2 + a, 3 - a, (x_at[a], gy))

    def c_copy(a, b):
        slot = 4 + 2 * a + b
        return remote(
            c_send.at[a, b], c_recv.at[1 - a, 1 - b], slot, 11 - slot, (x_at[a], y_at[b])
        )

    def send(present, copy, *known):
        @pl.when(present)
        def _():
            for number in known:
                pl.semaphore_wait(known_sem.at[number], 1)
            copy.start()

    def stage_y(side):
        near, far = ((0, 1), (SIDE - 1, SIDE - 2))[side]
        own(near)
        own(far)
        parts = (
            head[near],
            temp[near],
            category[near].astype(F32),
            ice[near],
            face(conduct[near], head[near], conduct[far], head[far]),
            temp[far],
        )
        for number, part in enumerate(parts):
            y_send[side, pl.ds(number * SIDE, SIDE), :] = part
        for a, x in enumerate((0, SIDE - 1)):
            for field, part in enumerate((head[near], temp[near], conduct[near], conduct[near])):
                c_send[a, side, pl.ds(field, 1), :] = part[x : x + 1, :]

    stage_y(1)
    for a in range(2):
        send(both[a][1], c_copy(a, 1))
    send(has_y[1], y_copy(1))

    edge = {}
    for x in (0, 1, SIDE - 2, SIDE - 1):
        h, t, c = tile(head_a, x), tile(temp_a, x), tile(cat_a, x)
        i = tile(ice_a, x).astype(F32)
        k = conductivity(h, t, lookup(c, ks_s), lookup(c, alpha_s), i)
        edge[x] = (h, t, c.astype(F32), i, k)
    for side, (near, far) in enumerate(((0, 1), (SIDE - 1, SIDE - 2))):
        inner, outer = edge[far], edge[near]
        parts = (*outer[:4], face(outer[4], outer[0], inner[4], inner[0]), inner[1])
        for number, part in enumerate(parts):
            x_send[side, pl.ds(number * SIDE, SIDE), :] = part
    send(has_x[1], x_copy(1))
    stage_y(0)
    send(has_x[0], x_copy(0), BEFORE)
    send(both[1][0], c_copy(1, 0), CROSS)
    send(has_y[0], y_copy(0), BELOW)

    @pl.when(is_hub)
    def _():
        for peer in peers:
            tell(ALL, (gx, peer))

    send(both[0][0], c_copy(0, 0), DIAGONAL)

    for copy in params[2:]:
        copy.wait()

    x_open = (jnp.logical_or(row > 0, has_x[0]), jnp.logical_or(row < SIDE - 1, has_x[1]))
    y_open = (jnp.logical_or(row > 0, has_y[0]), jnp.logical_or(row < SIDE - 1, has_y[1]))

    for y in range(2, SIDE - 2):
        own(y)

    def arrived(a, b):
        slot = 4 + 2 * a + b
        return remote(c_send.at[a, b], c_recv.at[a, b], slot, slot, (gx, gy_lo))

    x_waits = [
        (has_x[a], remote(x_send.at[a], x_recv.at[a], 2 + a, 2 + a, (gx, gy_lo)))
        for a in range(2)
    ]
    y_waits = [(both[a][b], arrived(a, b)) for a in range(2) for b in range(2)]
    y_waits += [
        (has_y[b], remote(y_send.at[b], y_recv.at[b], b, b, (gx, gy_lo))) for b in range(2)
    ]

    def receive(waits):
        for present, copy in waits:

            @pl.when(present)
            def _():
                copy.wait_recv()

    def along_rows(value, before, after):
        return (
            jnp.where(first, before, pltpu.roll(value, 1, 0)),
            jnp.where(last, after, pltpu.roll(value, SIDE - 1, 0)),
        )

    def change_rows(head_, conduct_, temp_, ends, opened):
        (h_lo, t_lo, k_lo), (h_hi, t_hi, k_hi) = ends
        heads = along_rows(head_, h_lo, h_hi)
        temps = along_rows(temp_, t_lo, t_hi)
        conducts = along_rows(conduct_, k_lo, k_hi)
        total = sum(
            jnp.where(opened[s], (conduct_ + conducts[s]) * (heads[s] - head_), 0.0)
            for s in range(2)
        )
        return total, temps[0] + temps[1]

    def y_part(side, number):
        return y_recv[side, pl.ds(number * SIDE, SIDE), :]

    def x_part(side, number):
        return x_recv[side, pl.ds(number * SIDE, SIDE), :]

    def warm_if(present, value):
        return jnp.where(present, value, 0.0)

    def corner(xs, ys):
        return (
            c_recv[xs, ys, pl.ds(0, 1), :],
            warm_if(jnp.logical_and(has_x[xs], has_y[ys]), c_recv[xs, ys, pl.ds(1, 1), :]),
            c_recv[xs, ys, pl.ds(2, 1), :],
        )

    def read_ghost(part_of, side, present):
        h, t, c, i = (part_of(side, number) for number in range(4))
        k_s, a = lookup(c, ks_s), lookup(c, alpha_s)
        far = tuple(part_of(side, number) for number in range(4, 6))
        return h, warm_if(present, t), conductivity(h, t, k_s, a, i), k_s, a, i, far

    def step(h, t, change, warm):
        return h + 0.5 * change, t + DIFFUSE * (warm - 6.0 * t)

    def ghost_base(cell, inner):
        h, t, k, far = cell[0], cell[1], cell[2], cell[6]
        change, warm = vertical(h, t, k, lane)
        change = change + far[0] + face(k, h, inner[2], inner[0])
        return change, warm + far[1] + inner[1]

    def ghost_step(cell, base, ends, opened, present):
        h, t, k, k_s, a, i, _ = cell
        rows, rows_warm = change_rows(h, k, t, ends, opened)
        h, t = step(h, t, base[0] + rows, base[1] + rows_warm)
        return h, warm_if(present, t), conductivity(h, t, k_s, a, i)

    def keep(slot, cells):
        for side in range(2):
            for field in range(3):
                ghost[slot + side, field] = cells[side][field]

    def base_of(y, h, t, k, slot):
        ends = tuple(
            tuple(ghost[slot + side, field, pl.ds(y, 1), :] for field in range(3))
            for side in range(2)
        )
        change, warm = vertical(h[y], t[y], k[y], lane)
        rows, rows_warm = change_rows(h[y], k[y], t[y], ends, x_open)
        return change + rows, warm + rows_warm

    def plane_step(y, h, t, k, base, faces):
        for edge_ in (y, y + 1):
            if edge_ not in faces:
                value = face(k[edge_ - 1], h[edge_ - 1], k[edge_], h[edge_])
                if edge_ in (0, SIDE):
                    value = jnp.where(has_y[edge_ // SIDE], value, 0.0)
                faces[edge_] = value
        return step(
            h[y],
            t[y],
            base[0] + faces[y + 1] - faces[y],
            base[1] + t[y - 1] + t[y + 1],
        )

    planes_all = gy_count * SIDE

    def view_planes(view, planes, theta):
        clear = depth = None
        sums = [None] * 3
        for y in planes:
            shift = skew_s[view] * ((gy * SIDE + y).astype(F32) - 0.5 * planes_all)
            wrapped = shift - DEPTH * jnp.floor(shift * (1.0 / DEPTH))
            base = jnp.floor(wrapped)
            part = wrapped - base
            turn = lax.rem(2 * DEPTH - base.astype(jnp.int32), DEPTH)
            lower = pltpu.roll(theta[y], turn, 1)
            upper = pltpu.roll(theta[y], lax.rem(turn + DEPTH - 1, DEPTH), 1)
            sample = (1.0 - part) * lower + part * upper
            optical = sample * (8.0 / planes_all)
            passed = jnp.exp(-optical)
            after = passed if clear is None else clear * passed
            weight = (1.0 if clear is None else clear) - after
            clear = after
            depth = optical if depth is None else depth + optical
            for color in range(3):
                term = weight * jnp.tanh((0.5 * steep_s[color]) * (sample - mid_s[color]))
                sums[color] = term if sums[color] is None else sums[color] + term
        return clear, sums, depth

    theta = {}

    def finish(y, h, t):
        head_v[pl.ds(y, SIDE, stride=SIDE), :] = h
        temp_v[pl.ds(y, SIDE, stride=SIDE), :] = t
        theta[y] = 0.05 + 0.4 * jnp.exp(0.8 * jnp.minimum(h, 0.0))

    receive(x_waits)
    x_ghost = [read_ghost(x_part, side, has_x[side]) for side in range(2)]
    keep(0, x_ghost)
    bases = [base_of(y, head, temp, conduct, 0) for y in range(SIDE)]
    faces, head_1, temp_1, conduct_1 = {}, {}, {}, {}

    def first_step(y):
        head_1[y], temp_1[y] = plane_step(y, head, temp, conduct, bases[y], faces)
        conduct_1[y] = conductivity(head_1[y], temp_1[y], ks[y], alpha[y], ice[y])

    for y in range(1, SIDE - 1):
        first_step(y)
    x_bases = [
        ghost_base(x_ghost[side], (edge[x][0], edge[x][1], edge[x][4]))
        for side, x in ((0, 0), (1, SIDE - 1))
    ]
    nothing = jnp.zeros((1, DEPTH), F32)
    keep(
        2,
        [
            ghost_step(x_ghost[side], x_bases[side], ((nothing,) * 3,) * 2, y_open, has_x[side])
            for side in range(2)
        ],
    )
    bases_1 = {y: base_of(y, head_1, temp_1, conduct_1, 2) for y in range(1, SIDE - 1)}
    faces_1 = {}
    middle = range(2, SIDE - 2)
    for y in middle:
        finish(y, *plane_step(y, head_1, temp_1, conduct_1, bases_1[y], faces_1))
    middles = [view_planes(view, middle, theta) for view in range(VIEWS)]

    receive(y_waits)
    y_ghost = [read_ghost(y_part, side, has_y[side]) for side in range(2)]
    for side, y in ((0, -1), (1, SIDE)):
        head[y], temp[y], conduct[y] = y_ghost[side][:3]
    for y in (0, SIDE - 1):
        first_step(y)
    for side, y, out in ((0, 0, -1), (1, SIDE - 1, SIDE)):
        head_1[out], temp_1[out], conduct_1[out] = ghost_step(
            y_ghost[side],
            ghost_base(y_ghost[side], (head[y], temp[y], conduct[y])),
            (corner(0, side), corner(1, side)),
            x_open,
            has_y[side],
        )
    keep(
        4,
        [
            ghost_step(
                x_ghost[side],
                x_bases[side],
                (corner(side, 0), corner(side, 1)),
                y_open,
                has_x[side],
            )
            for side in range(2)
        ],
    )
    for y in (0, SIDE - 1):
        bases_1[y] = base_of(y, head_1, temp_1, conduct_1, 4)
    for y in (0, 1, SIDE - 2, SIDE - 1):
        finish(y, *plane_step(y, head_1, temp_1, conduct_1, bases_1[y], faces_1))

    layers = []
    for view in range(VIEWS):
        clear_a, sums_a, depth_a = view_planes(view, (0, 1), theta)
        clear_b, sums_b, depth_b = middles[view]
        clear_c, sums_c, depth_c = view_planes(view, (SIDE - 2, SIDE - 1), theta)
        opaque = 1.0 - clear_a * (clear_b * clear_c)
        for color in range(3):
            total = sums_a[color] + clear_a * (sums_b[color] + clear_b * sums_c[color])
            layers.append(0.5 * (opaque + total))
        layers.append(depth_a + depth_b + depth_c)
    piece_send[...] = jnp.transpose(jnp.concatenate(layers, 0))

    among_late = jnp.where(gy < LATE, 1, 0)

    def exchange(src, dst, device):
        return pltpu.make_async_remote_copy(
            src_ref=src,
            dst_ref=dst,
            send_sem=local_sem.at[6],
            recv_sem=piece_recv_sem.at[among_late],
            device_id=device,
            device_id_type=MESH,
        )

    plain = jnp.logical_not(jnp.logical_or(is_hub, is_late))

    def give(peer):
        exchange(
            piece_send.at[pl.ds(pl.multiple_of(peer * SIDE, SIDE), SIDE)],
            piece_recv.at[gy],
            (gx, peer),
        ).start()

    @pl.when(plain)
    def _():
        pl.semaphore_wait(known_sem.at[MOST], 1)

    @pl.when(is_late)
    def _():
        pl.semaphore_wait(known_sem.at[ALL], 1)

    @pl.when(is_hub)
    def _():
        give(HUB - 1)

    soon = [(2, 3), (1, 3), (3, 3), (2, 0), (1, 0), (3, 0)]
    for dx, dy in soon + [d for d in shifts if d not in soon]:
        peer = lax.rem(px + dx, 4) * 4 + lax.rem(py + dy, 4)

        @pl.when(peer != HUB - 1)
        def _():
            give(peer)

    @pl.when(plain)
    def _():
        pl.semaphore_wait(known_sem.at[ALL], 1)
        give(HUB - 1)

    piece_recv[gy] = piece_send[pl.ds(pl.multiple_of(gy * SIDE, SIDE), SIDE), :]

    view_of = lax.div(lane, 4 * SIDE)
    kind_of = lax.rem(lax.div(lane, SIDE), 4)
    ranks = []
    for group in range(GROUPS):
        rank = jnp.full((SIDE, DEPTH), order_s[0, group], jnp.int32)
        for view in range(1, VIEWS):
            rank = jnp.where(view_of == view, order_s[view, group], rank)
        ranks.append(rank)
    is_depth = kind_of == 3

    def arrive(number, tiles):
        slots = piece_recv.at[pl.ds(0, tiles)]
        pltpu.make_async_remote_copy(
            src_ref=slots,
            dst_ref=slots,
            send_sem=local_sem.at[6],
            recv_sem=piece_recv_sem.at[number],
            device_id=(gx, gy_lo),
            device_id_type=MESH,
        ).wait_recv()

    depths, fronts = {}, {}

    def place(group):
        value = jnp.where(is_depth, piece_recv[group], 0.0)
        value = value + pltpu.roll(value, DEPTH - SIDE, 1)
        depths[group] = value + pltpu.roll(value, DEPTH - 2 * SIDE, 1)
        total = jnp.zeros((SIDE, DEPTH), F32)
        for other in fronts:
            before = ranks[other] < ranks[group]
            total = total + jnp.where(before, depths[other], 0.0)
            fronts[other] = fronts[other] + jnp.where(before, 0.0, depths[group])
        fronts[group] = total

    for number, groups, tiles in ((0, range(LATE, GROUPS), GROUPS - LATE), (1, range(LATE), LATE)):
        own_late = among_late == number

        @pl.when(own_late)
        def _():
            arrive(number, tiles - 1)

        @pl.when(jnp.logical_not(own_late))
        def _():
            arrive(number, tiles)

        for group in groups:
            place(group)
    color = sum(jnp.exp(-fronts[group]) * piece_recv[group] for group in range(GROUPS))
    opaque = 1.0 - jnp.exp(-sum(depths.values()))
    image_v[...] = jnp.transpose(jnp.where(is_depth, opaque, color))
    for present, copy in x_waits + y_waits:

        @pl.when(present)
        def _():
            copy.wait_send()

    sent = piece_recv.at[pl.ds(0, GROUPS - 1)]
    pltpu.make_async_remote_copy(
        src_ref=sent,
        dst_ref=sent,
        send_sem=local_sem.at[6],
        recv_sem=piece_recv_sem.at[0],
        device_id=(gx, gy_lo),
        device_id_type=MESH,
    ).wait_send()


def put_out(head_v, temp_v, image_v, head_out, temp_out, image_out, sem):
    copies = [
        pltpu.make_async_copy(src, dst, sem.at[number])
        for number, (src, dst) in enumerate(
            ((image_v, image_out), (head_v, head_out), (temp_v, temp_out))
        )
    ]
    for copy in copies:
        copy.start()
    for copy in copies:
        copy.wait()


def shards(head, temp, category, ice, *params):
    gx_count, gy_count = lax.axis_size("gx"), lax.axis_size("gy")
    rows = SIDE * SIDE
    flat = [a.reshape(rows, DEPTH) for a in (head, temp, category, ice)]
    vmem = pltpu.VMEM
    dma = pltpu.SemaphoreType.DMA
    shapes = ((rows, DEPTH), (rows, DEPTH), (DEPTH, SIDE))
    results = pl.pallas_call(
        functools.partial(kernel, gx_count, gy_count),
        out_shape=tuple(pltpu.VMEM(shape, F32) for shape in shapes),
        in_specs=[pl.BlockSpec(memory_space=pl.ANY)] * 10,
        out_specs=[pl.BlockSpec(memory_space=pltpu.VMEM)] * 3,
        scratch_shapes=[
            vmem((rows, DEPTH), F32),
            vmem((rows, DEPTH), F32),
            vmem((rows, DEPTH), jnp.int32),
            vmem((rows, DEPTH), jnp.int32),
            pltpu.SMEM((SOILS,), F32),
            pltpu.SMEM((SOILS,), F32),
            pltpu.SMEM((VIEWS,), F32),
            pltpu.SMEM((3,), F32),
            pltpu.SMEM((3,), F32),
            pltpu.SMEM((VIEWS, GROUPS), jnp.int32),
            vmem((2, 6 * SIDE, DEPTH), F32),
            vmem((2, 6 * SIDE, DEPTH), F32),
            vmem((2, 6 * SIDE, DEPTH), F32),
            vmem((2, 6 * SIDE, DEPTH), F32),
            vmem((2, 2, 4, DEPTH), F32),
            vmem((2, 2, 4, DEPTH), F32),
            vmem((6, 3, SIDE, DEPTH), F32),
            vmem((DEPTH, DEPTH), F32),
            vmem((GROUPS, SIDE, DEPTH), F32),
            dma((12,)),
            dma((8,)),
            pltpu.SemaphoreType.REGULAR((6,)),
            dma((2,)),
        ],
        compiler_params=pltpu.CompilerParams(collective_id=0, has_side_effects=True),
        name="step_and_view",
    )(*flat, *params)
    head, temp, image = pl.pallas_call(
        put_out,
        out_shape=tuple(jax.ShapeDtypeStruct(shape, F32) for shape in shapes),
        in_specs=[pl.BlockSpec(memory_space=pltpu.VMEM)] * 3,
        out_specs=[pl.BlockSpec(memory_space=pl.ANY)] * 3,
        scratch_shapes=[dma((3,))],
        name="put_out",
    )(*(pltpu.with_memory_space_constraint(r, pltpu.VMEM) for r in results))
    shape = (SIDE, SIDE, DEPTH)
    return head.reshape(shape), temp.reshape(shape), image.reshape(VIEWS, 4, SIDE, SIDE)


def solution(mesh):
    block = P("gx", "gy", None)
    return jax.shard_map(
        shards,
        mesh=mesh,
        in_specs=(block,) * 4 + (P(),) * 6,
        out_specs=(block, block, P(None, None, "gx", "gy")),
        check_vma=False,
    )
```
